8 devices in a mesh: rep: 2 (over y, z), dp: 4 (over x, core).
Axes of the slice: x: 2, y: 2, z: 1, core: 2. Of those that a mesh axis runs over, the one named last changes fastest.
Arguments:
- x: bfloat16 [8, 2048, 1536], P(('rep', 'dp')), parts along dimension 0
- dy: bfloat16 [8, 2048, 1536], P(('rep', 'dp')), parts along dimension 0
- w_gate: bfloat16 [2, 1536, 3584], P(None, 'dp')
- w_up: bfloat16 [2, 1536, 3584], P(None, 'dp')
- w_down: bfloat16 [2, 3584, 1536], P(None, 'dp')
- m_w_gate: float32 [2, 1536, 3584], P(None, 'dp')
- m_w_up: float32 [2, 1536, 3584], P(None, 'dp')
- m_w_down: float32 [2, 3584, 1536], P(None, 'dp')
- v_w_gate: float32 [2, 1536, 3584], P(None, 'dp')
- v_w_up: float32 [2, 1536, 3584], P(None, 'dp')
- v_w_down: float32 [2, 3584, 1536], P(None, 'dp')
Outputs:
- output 1: bfloat16 [4, 1536, 3584], P('rep', 'dp'), parts along dimension 0
- output 2: bfloat16 [4, 1536, 3584], P('rep', 'dp'), parts along dimension 0
- output 3: bfloat16 [4, 3584, 1536], P('rep', 'dp'), parts along dimension 0
- output 4: float32 [4, 1536, 3584], P('rep', 'dp'), parts along dimension 0
- output 5: float32 [4, 1536, 3584], P('rep', 'dp'), parts along dimension 0
- output 6: float32 [4, 3584, 1536], P('rep', 'dp'), parts along dimension 0
- output 7: float32 [4, 1536, 3584], P('rep', 'dp'), parts along dimension 0
- output 8: float32 [4, 1536, 3584], P('rep', 'dp'), parts along dimension 0
- output 9: float32 [4, 3584, 1536], P('rep', 'dp'), parts along dimension 0
There are 2 independent parts. The reference program is written for one: setup_inputs(seed, part) draws one part's arguments, and reference() takes and returns one part's arrays. A program takes and returns all parts, laid end to end along the dimension named above; an argument that names none is the same for every part.
All inputs are finite; a program needn't handle non-finite values.
Results may differ from the reference program's by a relative error of at most 0.022.
Values are sent between devices in bfloat16 or wider.
A program may use at most 2 GiB of HBM per device.

```python
import jax
import jax.numpy as jnp
from jax import lax

SEQUENCES = 4
TOKENS = 2048
D = 1536
FF = 3584
LAYERS = 2
NAMES = ("w_gate", "w_up", "w_down")
SHAPES = {"w_gate": (LAYERS, D, FF), "w_up": (LAYERS, D, FF), "w_down": (LAYERS, FF, D)}


def bump(key, n, height):
    away = (jnp.arange(n, dtype=jnp.int32) - jax.random.randint(key, (), 0, n, jnp.int32)) % n
    return jnp.where(away < n // 8, height, 1.0)


def together(key, own, strength):
    shared = jax.random.normal(key, own.shape[1:], jnp.float32)
    return (own + strength * shared) * lax.rsqrt(1 + strength * strength)


def setup_inputs(seed: int = 0, part: int = 0) -> dict:
    kx, kdy, ka, kb, kz, kf, kh, kl, *keys = jax.random.split(jax.random.key(seed), 8 + 3 * len(NAMES))
    kx, kdy, ka, kb = (jax.random.fold_in(k, part) for k in (kx, kdy, ka, kb))
    kw, km, kv = (keys[i::3] for i in range(3))
    shape = (SEQUENCES, TOKENS, D)
    much_x, much_dy = jax.random.uniform(kz, (2,), jnp.float32, 0.0, 1.0)
    loud = 2.0 ** jax.random.uniform(jax.random.fold_in(kz, 1), (), jnp.float32, -1.0, 2.0)
    layers = 2.0 ** jax.random.uniform(kl, (LAYERS, 1, 1), jnp.float32, -1.0, 1.0)
    x = together(ka, jax.random.normal(kx, shape, jnp.float32), much_x) * bump(kf, D, 4.0)
    dy = together(kb, jax.random.normal(kdy, shape, jnp.float32), much_dy)
    drawn = {"x": x.astype(jnp.bfloat16), "dy": (loud * dy * (SEQUENCES * TOKENS) ** -0.5).astype(jnp.bfloat16)}
    for key, name in zip(kw, NAMES, strict=True):
        w = jax.random.normal(key, SHAPES[name], jnp.float32) * SHAPES[name][1] ** -0.5
        drawn[name] = (w * {"w_gate": 1.0, "w_up": bump(kh, FF, 4.0), "w_down": layers}[name]).astype(jnp.bfloat16)
    for key, name in zip(km, NAMES, strict=True):
        drawn[f"m_{name}"] = 0.1 * jax.random.normal(key, SHAPES[name], jnp.float32)
    for key, name in zip(kv, NAMES, strict=True):
        drawn[f"v_{name}"] = jax.random.uniform(key, SHAPES[name], jnp.float32, 0.005, 0.015)
    return drawn


def matmul(a, w):
    return jnp.dot(a, w, preferred_element_type=jnp.float32).astype(jnp.bfloat16)


def normed(h):
    wide = h.astype(jnp.float32)
    scale = lax.rsqrt(jnp.mean(wide**2, -1, keepdims=True) + 1e-6)
    return (wide * scale).astype(jnp.bfloat16)


def layer(h, w):
    a = normed(h)
    gate = jnp.dot(a, w["w_gate"], preferred_element_type=jnp.float32)
    up = jnp.dot(a, w["w_up"], preferred_element_type=jnp.float32)
    return h + matmul((jax.nn.silu(gate) * up).astype(jnp.bfloat16), w["w_down"])


def adamw(w, m, v, g):
    m = 0.9 * m + 0.1 * g
    v = 0.95 * v + 0.05 * g * g
    step = m * lax.rsqrt(v + 1e-8) + 0.1 * w
    return (w - 0.02 * step).astype(jnp.bfloat16), m, v


def clipped(gradients, sum_of_squares, count):
    factor = jnp.minimum(1.0, 0.5 * lax.rsqrt(sum_of_squares / count + 1e-30))
    return [g * factor for g in gradients]


def stack(weights, h):
    return lax.scan(lambda h, w: (layer(h, w), None), h, weights)[0]


def reference(x, dy, w_gate, w_up, w_down, m_w_gate, m_w_up, m_w_down, v_w_gate, v_w_up, v_w_down):
    weights = dict(zip(NAMES, (w_gate, w_up, w_down), strict=True))

    def take(so_far, sequence):
        h, by_y = sequence
        _, back = jax.vjp(lambda w: stack(w, h), weights)
        return jax.tree.map(lambda total, term: total + term.astype(jnp.float32), so_far, back(by_y)[0]), None

    none_yet = {name: jnp.zeros(w.shape, jnp.float32) for name, w in weights.items()}
    by_weights, _ = lax.scan(take, none_yet, (x, dy))
    gradients = [by_weights[name].astype(jnp.bfloat16).astype(jnp.float32) for name in NAMES]
    gradients = clipped(gradients, sum(jnp.sum(g * g) for g in gradients), sum(g.size for g in gradients))
    new = [
        adamw(w.astype(jnp.float32), m, v, g)
        for w, m, v, g in zip((w_gate, w_up, w_down), (m_w_gate, m_w_up, m_w_down), (v_w_gate, v_w_up, v_w_down), gradients, strict=True)
    ]
    return tuple(one[which] for which in range(3) for one in new)
```

```python
import functools

import jax
import jax.numpy as jnp
from jax import lax
from jax.experimental import pallas as pl
from jax.experimental.pallas import tpu as pltpu
from jax.sharding import PartitionSpec as P


F32, BF16 = jnp.float32, jnp.bfloat16
OVER_X = [(0, 2), (2, 0), (1, 3), (3, 1)]
OVER_CORE = [(0, 1), (1, 0), (2, 3), (3, 2)]
OVER_Y = [(0, 1), (1, 0)]


def normed(h):
    wide = h.astype(F32)
    scale = lax.rsqrt(jnp.mean(wide**2, -1, keepdims=True) + 1e-6)
    return (wide * scale).astype(BF16)


def activated(gate, up):
    return (jax.nn.silu(gate) * up).astype(BF16)


def dot(a, b, dims):
    return lax.dot_general(a, b, (dims, ((), ())), preferred_element_type=F32)


def adamw(w, m, v, g):
    m = 0.9 * m + 0.1 * g
    v = 0.95 * v + 0.05 * g * g
    step = m * lax.rsqrt(v + 1e-8) + 0.1 * w
    return (w - 0.02 * step).astype(BF16), m, v


def others(d):
    x, c = d // 2, d % 2
    return d, 2 * x + 1 - c, 2 * (1 - x) + c, 2 * (1 - x) + 1 - c


def assemble_kernel(number, rows, own, own_c, rx, ry, rx_c, ry_c, out, buf, sem_in, sem_out):
    d, r = lax.axis_index("dp"), lax.axis_index("rep")
    half = rows // 2
    own_i, core_i, x_i, xc_i = others(d)
    at = lambda i, n: pl.ds(pl.multiple_of(i, 16), n)
    moves = [
        (own.at[number], own_i * rows, rows),
        (own_c.at[number], core_i * rows, rows),
        (rx, x_i * rows + r * half, half),
        (ry, x_i * rows + (1 - r) * half, half),
        (rx_c, xc_i * rows + r * half, half),
        (ry_c, xc_i * rows + (1 - r) * half, half),
    ]
    ins = [pltpu.make_async_copy(src, buf.at[at(i, n)], sem_in.at[k]) for k, (src, i, n) in enumerate(moves)]
    outs = [pltpu.make_async_copy(buf.at[at(i, n)], out.at[at(i, n)], sem_out.at[k]) for k, (src, i, n) in enumerate(moves)]
    for one in ins:
        one.start()
    for one, two in zip(ins, outs):
        one.wait()
        two.start()
    for one in outs:
        one.wait()


def assembled(number, own, own_c, rx, ry, rx_c, ry_c):
    _, rows, cols = own.shape
    any_space = pl.BlockSpec(memory_space=pl.ANY)
    return pl.pallas_call(
        functools.partial(assemble_kernel, number, rows),
        out_shape=jax.ShapeDtypeStruct((4 * rows, cols), BF16),
        in_specs=[any_space] * 6,
        out_specs=any_space,
        scratch_shapes=[pltpu.VMEM((4 * rows, cols), BF16), pltpu.SemaphoreType.DMA((6,)), pltpu.SemaphoreType.DMA((6,))],
        compiler_params=pltpu.CompilerParams(vmem_limit_bytes=24 << 20),
        cost_estimate=pl.CostEstimate(flops=10**9, bytes_accessed=8 * 4 * rows * cols, transcendentals=0),
        name="assemble",
    )(own, own_c, rx, ry, rx_c, ry_c)


def solution(mesh):
    def step(x, dy, *arrays):
        weights, m, v = (arrays[i : i + 3] for i in (0, 3, 6))
        d, r = lax.axis_index("dp"), lax.axis_index("rep")
        own_i, core_i, x_i, xc_i = others(d)
        layers = weights[0].shape[0]

        from_core = [lax.ppermute(w, "dp", OVER_CORE) for w in weights]

        def across(i, number):
            rows, cols = weights[i].shape[1:]
            half = rows // 2
            mine = lax.dynamic_slice(weights[i], (number, r * half, 0), (1, half, cols))[0]
            return lax.ppermute(mine, "dp", OVER_X)

        halves = {(i, number): across(i, number) for number in range(layers) for i in range(3)}

        def fetched(i, number, *behind):
            rx = halves[i, number]
            if behind:
                rx = lax.optimization_barrier((rx, *behind))[0]
            ry = lax.ppermute(rx, "rep", OVER_Y)
            rx_c = lax.ppermute(rx, "dp", OVER_CORE)
            ry_c = lax.ppermute(ry, "dp", OVER_CORE)
            return assembled(number, weights[i], from_core[i], rx, ry, rx_c, ry_c)

        last = []

        def ordered(*some):
            out = lax.optimization_barrier((*some, *last))[: len(some)] if last else some
            return out[0] if len(some) == 1 else out

        def noted(one):
            last[:] = [one]
            return one

        token = ((0,), (0,))

        def term(left, right, i, arrived=None, kind=BF16):
            rows = left.shape[1] // 4
            left = ordered(lax.dynamic_slice(left, (0, i * rows), (left.shape[0], rows)))
            out = dot(left, right, token)
            if arrived is not None:
                out = out + arrived.astype(F32)
            return out.astype(kind)

        kept, full = [], []
        h = x[0]
        for number in range(layers):
            a, back_norm = jax.vjp(normed, h)
            if number == 0:
                w_gate, w_up = fetched(0, 0), fetched(1, 0)
            gate = dot(a, w_gate, ((1,), (0,)))
            if number == 0:
                w_down = fetched(2, 0, gate)
            else:
                w_down = fetched(2, 1, gate)
            up = dot(ordered(a, gate)[0], w_up, ((1,), (0,)))
            hidden, back_act = jax.vjp(activated, gate, up)
            kept.append((a, back_norm, hidden, back_act))
            full.append((w_gate, w_up, w_down))
            if number == 0:
                w_gate = fetched(0, 1, hidden)
                h = h + dot(hidden, w_down, ((1,), (0,))).astype(BF16)
                w_up = fetched(1, 1, h)
        noted(hidden)

        by_h, mine, late = dy[0], [[None] * 3 for _ in range(layers)], []
        for number in reversed(range(layers)):
            w_gate, w_up, w_down = full[number]
            a, back_norm, hidden, back_act = kept[number]

            def start(i, left, right, number=number):
                a_mine = noted(term(left, right, xc_i))
                a_there = lax.ppermute(a_mine, "dp", OVER_CORE)
                b_mine = noted(term(left, right, core_i))
                b_there = lax.ppermute(b_mine, "dp", OVER_CORE)
                sent = noted(term(left, right, x_i, a_there))
                from_x = lax.ppermute(sent, "dp", OVER_X)
                late.append((i, number, from_x, lambda: noted(term(left, right, own_i, b_there, F32))))

            start(2, hidden, by_h)
            by_here = ordered(by_h)
            by_hidden = dot(by_here, w_down, ((1,), (1,))).astype(BF16)
            by_gate, by_up = (noted(t.astype(BF16)) for t in back_act(by_hidden))
            start(0, a, by_gate)
            start(1, a, by_up)
            if number > 0:
                by_a = noted(dot(ordered(by_gate), w_gate, ((1,), (1,))).astype(BF16))
                by_a = by_a + dot(ordered(by_up), w_up, ((1,), (1,))).astype(BF16)
                by_h = noted(by_h + back_norm(by_a)[0])
        owns = lax.optimization_barrier([own() for _, _, _, own in late])
        for (i, number, from_x, _), own in zip(late, owns):
            mine[number][i] = (own + from_x.astype(F32)).astype(BF16)

        squares = sum(jnp.sum(jnp.square(g.astype(F32))) for gs in mine for g in gs)
        squares = lax.psum(squares, "dp")
        count = 4 * sum(g.size for gs in mine for g in gs)
        factor = jnp.minimum(1.0, 0.5 * lax.rsqrt(squares / count + 1e-30))
        new = []
        for i in range(3):
            g = jnp.stack([mine[number][i] for number in range(layers)]).astype(F32) * factor
            new.append(adamw(weights[i].astype(F32), m[i], v[i], g))
        return tuple(one[which] for which in range(3) for one in new)

    states, cut = P(("rep", "dp"), None, None), P(None, "dp", None)
    return jax.shard_map(
        step,
        mesh=mesh,
        in_specs=(states, states) + (cut,) * 9,
        out_specs=(P("rep", "dp", None),) * 9,
        check_vma=False,
    )
```

```python
import functools

import jax
import jax.numpy as jnp
from jax import lax
from jax.experimental import pallas as pl
from jax.experimental.pallas import tpu as pltpu
from jax.sharding import PartitionSpec as P


F32, BF16 = jnp.float32, jnp.bfloat16
OVER_X = [(0, 2), (2, 0), (1, 3), (3, 1)]
OVER_CORE = [(0, 1), (1, 0), (2, 3), (3, 2)]
OVER_Y = [(0, 1), (1, 0)]


def normed(h):
    wide = h.astype(F32)
    scale = lax.rsqrt(jnp.mean(wide**2, -1, keepdims=True) + 1e-6)
    return (wide * scale).astype(BF16)


def adamw(w, m, v, g):
    m = 0.9 * m + 0.1 * g
    v = 0.95 * v + 0.05 * g * g
    step = m * lax.rsqrt(v + 1e-8) + 0.1 * w
    return (w - 0.02 * step).astype(BF16), m, v


def others(d):
    x, c = d // 2, d % 2
    return d, 2 * x + 1 - c, 2 * (1 - x) + c, 2 * (1 - x) + 1 - c


def assemble_kernel(number, rows, own, own_c, rx, ry, rx_c, ry_c, out, buf, sem_in, sem_out):
    d, r = lax.axis_index("dp"), lax.axis_index("rep")
    half = rows // 2
    own_i, core_i, x_i, xc_i = others(d)
    at = lambda i, n: pl.ds(pl.multiple_of(i, 16), n)
    moves = [
        (own.at[number], own_i * rows, rows),
        (own_c.at[number], core_i * rows, rows),
        (rx, x_i * rows + r * half, half),
        (ry, x_i * rows + (1 - r) * half, half),
        (rx_c, xc_i * rows + r * half, half),
        (ry_c, xc_i * rows + (1 - r) * half, half),
    ]
    ins = [pltpu.make_async_copy(src, buf.at[at(i, n)], sem_in.at[k]) for k, (src, i, n) in enumerate(moves)]
    outs = [pltpu.make_async_copy(buf.at[at(i, n)], out.at[at(i, n)], sem_out.at[k]) for k, (src, i, n) in enumerate(moves)]
    for one in ins:
        one.start()
    for one, two in zip(ins, outs):
        one.wait()
        two.start()
    for one in outs:
        one.wait()


def assembled(number, own, own_c, rx, ry, rx_c, ry_c):
    _, rows, cols = own.shape
    any_space = pl.BlockSpec(memory_space=pl.ANY)
    return pl.pallas_call(
        functools.partial(assemble_kernel, number, rows),
        out_shape=jax.ShapeDtypeStruct((4 * rows, cols), BF16),
        in_specs=[any_space] * 6,
        out_specs=any_space,
        scratch_shapes=[pltpu.VMEM((4 * rows, cols), BF16), pltpu.SemaphoreType.DMA((6,)), pltpu.SemaphoreType.DMA((6,))],
        compiler_params=pltpu.CompilerParams(vmem_limit_bytes=VMEM),
        cost_estimate=pl.CostEstimate(flops=10**9, bytes_accessed=8 * 4 * rows * cols, transcendentals=0),
        name="assemble",
    )(own, own_c, rx, ry, rx_c, ry_c)


VMEM = 63 << 20


def call(kernel, out_shape, grid, in_specs, out_specs, flops, moved, prefetch=None, scratch=()):
    gs = pltpu.PrefetchScalarGridSpec(
        num_scalar_prefetch=0 if prefetch is None else 1,
        grid=grid,
        in_specs=in_specs,
        out_specs=out_specs,
        scratch_shapes=list(scratch),
    )
    return pl.pallas_call(
        kernel,
        out_shape=out_shape,
        grid_spec=gs,
        compiler_params=pltpu.CompilerParams(vmem_limit_bytes=VMEM),
        cost_estimate=pl.CostEstimate(flops=flops, bytes_accessed=moved, transcendentals=0),
    )


def shaped(shape, kind=BF16):
    return jax.ShapeDtypeStruct(shape, kind)


def resident(shape):
    return pl.BlockSpec(shape, lambda *_: (0,) * len(shape), pipeline_mode=pl.Buffered(1))


def turned_of(a):
    return a.astype(F32).T.astype(BF16)


def norm_kernel(x, a, a_t):
    out = normed(x[...])
    a[...] = out
    a_t[...] = turned_of(out)


def turn_kernel(x, x_t):
    x_t[...] = turned_of(x[...])


def back_norm_kernel(by_a, h, by_h, out, out_t):
    new = by_h[...] + jax.vjp(normed, h[...])[1](by_a[...])[0]
    out[...] = new
    out_t[...] = turned_of(new)


def by_rows(kernel, kinds, *arrays, bm=256):
    m, n = arrays[0].shape
    straight, across = pl.BlockSpec((bm, n), lambda i: (i, 0)), pl.BlockSpec((n, bm), lambda i: (0, i))
    return call(
        kernel, [shaped((n, m) if kind == "t" else (m, n)) for kind in kinds], (m // bm,), [straight] * len(arrays),
        [across if kind == "t" else straight for kind in kinds], 10**9, 2 * m * n * (len(arrays) + len(kinds)),
    )(*arrays)


def gate_up_kernel(number, width, at, a, *refs):
    sources, outs, (buf, sem) = (refs[:4], refs[4:8]), refs[-7:-2], refs[-2:]
    gate, up, hidden, wg, wu = outs
    t = pl.program_id(0)
    tile = gate.shape[1]
    rows = buf.shape[2] // 4
    here = lambda first: pl.ds(pl.multiple_of(first, 128), tile)

    def copies(t):
        slot = lax.rem(t, 2)
        out = []
        for p in range(2):
            own, own_c, rx, rx_c = sources[p]
            cut = [own.at[number, :, here(at[4] * width + t * tile)], own_c.at[number, :, here(at[4] * width + t * tile)]]
            cut += [rx.at[:, here(t * tile)], rx_c.at[:, here(t * tile)]]
            for k, src in enumerate(cut):
                dst = buf.at[slot, p, pl.ds(pl.multiple_of(at[k] * rows, rows), rows)]
                out.append(pltpu.make_async_copy(src, dst, sem.at[slot, p, k]))
        return out

    @pl.when(t == 0)
    def _():
        for one in copies(t):
            one.start()

    @pl.when(t + 1 < pl.num_programs(0))
    def _():
        for one in copies(t + 1):
            one.start()

    for one in copies(t):
        one.wait()
    slot = lax.rem(t, 2)
    wg[...] = buf[slot, 0]
    wu[...] = buf[slot, 1]
    g = jnp.dot(a[...], buf[slot, 0], preferred_element_type=F32)
    u = jnp.dot(a[...], buf[slot, 1], preferred_element_type=F32)
    gate[...] = g
    up[...] = u
    hidden[...] = (jax.nn.silu(g) * u).astype(BF16)


def gate_up(number, at, a, gates, ups, before=()):
    m, k = a.shape
    n, width = gates[0].shape[2], gates[2].shape[1]
    bn = 256
    tiles = width // bn
    any_space = pl.BlockSpec(memory_space=pl.ANY)
    place = lambda t, at: (0, at[4] * tiles + t)
    out, w = pl.BlockSpec((m, bn), place), pl.BlockSpec((k, bn), place)
    return pl.pallas_call(
        functools.partial(gate_up_kernel, number, width),
        out_shape=[shaped((m, n), F32), shaped((m, n), F32), shaped((m, n)), shaped((k, n)), shaped((k, n))],
        grid_spec=pltpu.PrefetchScalarGridSpec(
            num_scalar_prefetch=1,
            grid=(tiles,),
            in_specs=[resident((m, k))] + [any_space] * (8 + len(before)),
            out_specs=[out] * 3 + [w] * 2,
            scratch_shapes=[pltpu.VMEM((2, 2, k, bn), BF16), pltpu.SemaphoreType.DMA((2, 2, 4))],
        ),
        input_output_aliases={10 + i: i for i in range(len(before))},
        compiler_params=pltpu.CompilerParams(vmem_limit_bytes=VMEM),
        cost_estimate=pl.CostEstimate(flops=4 * m * width * k, bytes_accessed=10 * m * width + 4 * k * width, transcendentals=0),
        name="gate_up",
    )(at, a, *gates, *ups, *before)


def down_kernel(hidden, w, x, h, a, a_t):
    out = x[...] + jnp.dot(hidden[...], w[...], preferred_element_type=F32).astype(BF16)
    h[...] = out
    out = normed(out)
    a[...] = out
    a_t[...] = turned_of(out)


def down(hidden, w, x, bm=256):
    m, k = hidden.shape
    n = w.shape[1]
    out = pl.BlockSpec((bm, n), lambda i: (i, 0))
    return call(
        down_kernel, [shaped((m, n))] * 2 + [shaped((n, m))], (m // bm,),
        [pl.BlockSpec((bm, k), lambda i: (i, 0)), resident((k, n)), out], [out] * 2 + [pl.BlockSpec((n, bm), lambda i: (0, i))],
        2 * m * n * k, 2 * k * n + 2 * m * k,
    )(hidden, w, x)


NT = (((1,), (1,)), ((), ()))


def by_hidden_kernel(dy, w, gate, up, dg, du):
    by = lax.dot_general(dy[...], w[...], NT, preferred_element_type=F32).astype(BF16).astype(F32)
    g, u = gate[...], up[...]
    s = jax.nn.sigmoid(g)
    silu = g * s
    dg[...] = (by * u * (s + silu * (1 - s))).astype(BF16)
    du[...] = (by * silu).astype(BF16)


def by_hidden(dy, w, gate, up, bm=2048, bn=512):
    m, k = dy.shape
    n = w.shape[0]
    out = pl.BlockSpec((bm, bn), lambda j, i: (i, j))
    return call(
        by_hidden_kernel, [shaped((m, n))] * 2, (n // bn, m // bm),
        [resident((m, k)), pl.BlockSpec((bn, k), lambda j, i: (j, 0)), out, out], [out] * 2,
        2 * m * n * k, 12 * m * n,
    )(dy, w, gate, up)


def by_a_kernel(dg, du, wg, wu, out):
    one = lax.dot_general(dg[...], wg[...], NT, preferred_element_type=F32).astype(BF16)
    two = lax.dot_general(du[...], wu[...], NT, preferred_element_type=F32).astype(BF16)
    out[...] = one + two


def by_a(dg, du, wg, wu, bm=1024, bn=512):
    m, k = dg.shape
    n = wg.shape[0]
    lhs = pl.BlockSpec((bm, k), lambda i, j: (i, 0))
    w = pl.BlockSpec((bn, k), lambda i, j: (j, 0))
    return call(
        by_a_kernel, shaped((m, n)), (m // bm, n // bn), [lhs, lhs, w, w], pl.BlockSpec((bm, bn), lambda i, j: (i, j)),
        4 * m * n * k, 4 * m * k + 4 * n * k * (m // bm),
    )(dg, du, wg, wu)


TILE = 512


def exchange(d, src, dst, send_sem, recv_sem):
    return pltpu.make_async_remote_copy(
        src_ref=src, dst_ref=dst, send_sem=send_sem, recv_sem=recv_sem, device_id={"dp": others(d)[1]}, device_id_type=pl.DeviceIdType.MESH
    )


def greet(d):
    barrier = pltpu.get_barrier_semaphore()
    pl.semaphore_signal(barrier, inc=1, device_id={"dp": others(d)[1]}, device_id_type=pl.DeviceIdType.MESH)
    pl.semaphore_wait(barrier, 1)


def term_rows_kernel(left, right, send, own, full, there, send_sem, recv_sem):
    d = lax.axis_index("dp")
    own_i, core_i, x_i, xc_i = others(d)
    rows, tile = send.shape
    tiles = full.shape[1] // tile
    j = pl.program_id(0)
    cols = lambda k: pl.ds(pl.multiple_of(k * tile, tile), tile)
    at = lambda i: pl.ds(pl.multiple_of(i * rows, rows), rows)

    def copies(k):
        return [
            exchange(d, full.at[at(i), cols(k)], there.at[n, :, cols(k)], send_sem.at[n, k], recv_sem.at[n, k])
            for n, i in enumerate((core_i, xc_i))
        ]

    @pl.when(j == 0)
    def _():
        greet(d)

    @pl.when((j >= 1) & (j <= tiles))
    def _():
        for one in copies(j - 1):
            one.start()

    @pl.when(j < tiles)
    def _():
        full[:, cols(j)] = jnp.dot(left[...], right[...], preferred_element_type=F32).astype(BF16)

    @pl.when(j >= 2)
    def _():
        k = j - 2
        for one in copies(k):
            one.wait()
        own[...] = full[at(own_i), cols(k)].astype(F32) + there[0, :, cols(k)].astype(F32)
        send[...] = (full[at(x_i), cols(k)].astype(F32) + there[1, :, cols(k)].astype(F32)).astype(BF16)


def term_rows(left, right):
    m, k = left.shape
    n, rows, tiles = right.shape[1], m // 4, right.shape[1] // TILE
    out = pl.BlockSpec((rows, TILE), lambda j: (0, jnp.maximum(j - 2, 0)))
    return pl.pallas_call(
        term_rows_kernel,
        out_shape=[shaped((rows, n)), shaped((rows, n), F32)],
        grid=(tiles + 2,),
        in_specs=[resident((m, k)), pl.BlockSpec((k, TILE), lambda j: (0, jnp.minimum(j, tiles - 1)))],
        out_specs=[out, out],
        scratch_shapes=[pltpu.VMEM((m, n), BF16), pltpu.VMEM((2, rows, n), BF16), pltpu.SemaphoreType.DMA((2, tiles)), pltpu.SemaphoreType.DMA((2, tiles))],
        compiler_params=pltpu.CompilerParams(vmem_limit_bytes=VMEM, collective_id=0, has_side_effects=True),
        cost_estimate=pl.CostEstimate(flops=2 * m * n * k, bytes_accessed=2 * (m * k + k * n + m * n), transcendentals=0),
        name="term_rows",
    )(left, right)


def term_columns_kernel(left, right, send, own, full, there, send_sem, recv_sem):
    d = lax.axis_index("dp")
    x, c = d // 2, d % 2
    wide = send.shape[1]
    tile = right.shape[1]
    tiles = full.shape[1] // tile
    j = pl.program_id(0)

    def pieces(s):
        first, end = s * wide, (s + 1) * wide
        if s < 3:
            return [(first, wide, (end - 1) // tile)]
        cut = (tiles - 1) * tile
        return [(first, cut - first, (cut - 1) // tile), (cut, end - cut, tiles - 1)]

    def copies(s):
        out = []
        for p, (first, width, last) in enumerate(pieces(s)):
            n = jnp.where(x == s // 2, 0, 1)
            dst = there.at[n, :, pl.ds(first - s * wide, width)]
            out.append((last, exchange(d, full.at[:, pl.ds(first, width)], dst, send_sem.at[s, p], recv_sem.at[s, p])))
        return out

    @pl.when(j == 0)
    def _():
        greet(d)

    for s in range(4):
        for last, one in copies(s):

            @pl.when((j == last + 1) & (c != s % 2))
            def _(one=one):
                one.start()

    @pl.when(j < tiles)
    def _():
        here = pl.ds(pl.multiple_of(j * tile, tile), tile)
        full[:, here] = jnp.dot(left[...], right[...], preferred_element_type=F32).astype(BF16)

    @pl.when(j == tiles + 1)
    def _():
        for s in range(4):
            for last, one in copies(s):

                @pl.when(c != s % 2)
                def _(one=one):
                    one.wait_send()

                @pl.when(c == s % 2)
                def _(one=one):
                    one.wait_recv()

            @pl.when((c == s % 2) & (x == s // 2))
            def _(s=s):
                own[...] = full[:, pl.ds(s * wide, wide)].astype(F32) + there[0].astype(F32)

            @pl.when((c == s % 2) & (x != s // 2))
            def _(s=s):
                send[...] = (full[:, pl.ds(s * wide, wide)].astype(F32) + there[1].astype(F32)).astype(BF16)


def term_columns(left, right):
    m, k = left.shape
    n, wide, tiles = right.shape[1], right.shape[1] // 4, right.shape[1] // TILE
    return pl.pallas_call(
        term_columns_kernel,
        out_shape=[shaped((m, wide)), shaped((m, wide), F32)],
        grid=(tiles + 2,),
        in_specs=[resident((m, k)), pl.BlockSpec((k, TILE), lambda j: (0, jnp.minimum(j, tiles - 1)))],
        out_specs=[pl.BlockSpec((m, wide), lambda j: (0, 0))] * 2,
        scratch_shapes=[pltpu.VMEM((m, n), BF16), pltpu.VMEM((2, m, wide), BF16), pltpu.SemaphoreType.DMA((4, 2)), pltpu.SemaphoreType.DMA((4, 2))],
        compiler_params=pltpu.CompilerParams(vmem_limit_bytes=VMEM, collective_id=1, has_side_effects=True),
        cost_estimate=pl.CostEstimate(flops=2 * m * n * k, bytes_accessed=2 * (m * k + k * n + m * n), transcendentals=0),
        name="term_columns",
    )(left, right)


def turned_kernel(own, arrived, out, squares):
    g = (own[...] + arrived[...].astype(F32)).astype(BF16).astype(F32)

    @pl.when(pl.program_id(0) == 0)
    def _():
        squares[0, 0] = 0.0

    squares[0, 0] += jnp.sum(g * g)
    out[...] = g.T.astype(BF16)


def turned(own, arrived):
    m, n = own.shape
    bn = 128
    spec = pl.BlockSpec((m, bn), lambda j: (0, j))
    g, squares = pl.pallas_call(
        turned_kernel,
        out_shape=[shaped((n, m)), shaped((1, 1), F32)],
        grid=(n // bn,),
        in_specs=[spec, spec],
        out_specs=[pl.BlockSpec((bn, m), lambda j: (j, 0)), pl.BlockSpec(memory_space=pltpu.SMEM)],
        compiler_params=pltpu.CompilerParams(vmem_limit_bytes=VMEM),
        cost_estimate=pl.CostEstimate(flops=4 * m * n, bytes_accessed=8 * m * n, transcendentals=0),
        name="turned",
    )(own, arrived)
    return g, squares[0, 0]


def solution(mesh):
    def step(x, dy, *arrays):
        weights, m, v = (arrays[i : i + 3] for i in (0, 3, 6))
        d, r = lax.axis_index("dp"), lax.axis_index("rep")
        own_i, core_i, x_i, xc_i = others(d)
        layers = weights[0].shape[0]

        from_core = [lax.ppermute(w, "dp", OVER_CORE) for w in weights]

        def across(i, number):
            rows, cols = weights[i].shape[1:]
            if i == 2:
                mine = lax.dynamic_slice(weights[i], (number, r * (rows // 2), 0), (1, rows // 2, cols))[0]
            else:
                mine = lax.dynamic_slice(weights[i], (number, 0, r * (cols // 2)), (1, rows, cols // 2))[0]
            return lax.ppermute(mine, "dp", OVER_X)

        halves = {(i, number): across(i, number) for number in range(layers) for i in range(3)}

        def first(i, number, *behind):
            rx = halves[i, number]
            if behind:
                rx = lax.optimization_barrier((rx, *behind))[0]
            return lax.ppermute(rx, "dp", OVER_CORE)

        def second(i, number, *behind):
            rx = halves[i, number]
            if behind:
                rx = lax.optimization_barrier((rx, *behind))[0]
            ry = lax.ppermute(rx, "rep", OVER_Y)
            return ry, lax.ppermute(ry, "dp", OVER_CORE)

        def whole_down(number, behind):
            ry, ry_c = second(2, number, behind)
            return assembled(number, weights[2], from_core[2], halves[2, number], ry, first(2, number), ry_c)

        last = []

        def ordered(*some):
            out = lax.optimization_barrier((*some, *last))[: len(some)] if last else some
            return out[0] if len(some) == 1 else out

        def noted(one):
            last[:] = [one]
            return one

        at = jnp.stack([own_i, core_i, x_i, xc_i, r]).astype(jnp.int32)
        at_b = jnp.stack([own_i, core_i, x_i, xc_i, 1 - r]).astype(jnp.int32)

        def ab(number, a, behind):
            arrived = [(weights[i], from_core[i], halves[i, number], first(i, number, *behind[i])) for i in (0, 1)]
            outs = gate_up(number, at, a, *arrived)
            return outs, [(weights[i], from_core[i], *second(i, number, *behind[i])) for i in (0, 1)]

        a0, a0_t = by_rows(norm_kernel, " t", x[0])
        (dy_t,) = by_rows(turn_kernel, "t", dy[0])
        a0, a0_t, dy_t = lax.optimization_barrier((a0, a0_t, dy_t))
        outs, arrived = ab(0, a0, ((), ()))
        w_down0 = whole_down(0, outs[2])
        gate0, up0, hidden0, _, _ = gate_up(0, at_b, a0, *arrived, outs)
        h1, a1, a1_t = down(hidden0, w_down0, x[0])
        outs, arrived = ab(1, a1, ((hidden0,), (h1,)))
        w_down1 = whole_down(1, outs[2])
        gate1, up1, hidden1, w_gate1, w_up1 = gate_up(1, at_b, a1, *arrived, outs)
        noted(hidden1)

        mine, late = [[None] * 3 for _ in range(layers)], []

        def term(i, number, kernel, left, right):
            send, own = kernel(left, ordered(right))
            noted(send)
            late.append((i, number, lax.ppermute(send, "dp", OVER_X), own))

        term(2, 1, term_columns, dy_t, hidden1)
        by_gate, by_up = by_hidden(ordered(dy[0]), w_down1, gate1, up1)
        noted(by_gate)
        term(0, 1, term_rows, a1_t, by_gate)
        term(1, 1, term_rows, a1_t, by_up)
        by_in = by_a(ordered(by_gate), by_up, w_gate1, w_up1)
        by_h, by_h_t = by_rows(back_norm_kernel, " t", by_in, h1, dy[0])
        noted(by_h)
        term(2, 0, term_columns, by_h_t, hidden0)
        by_gate, by_up = by_hidden(ordered(by_h), w_down0, gate0, up0)
        noted(by_gate)
        term(0, 0, term_rows, a0_t, by_gate)
        term(1, 0, term_rows, a0_t, by_up)
        squares = 0.0
        for i, number, from_x, own in late:
            if i == 2:
                mine[number][i], more = turned(own, from_x)
            else:
                mine[number][i] = g = (own + from_x.astype(F32)).astype(BF16)
                more = jnp.sum(jnp.square(g.astype(F32)))
            squares += more

        squares = lax.psum(squares, "dp")
        count = 4 * sum(g.size for gs in mine for g in gs)
        factor = jnp.minimum(1.0, 0.5 * lax.rsqrt(squares / count + 1e-30))
        new = []
        for i in range(3):
            g = jnp.stack([mine[number][i] for number in range(layers)]).astype(F32) * factor
            new.append(adamw(weights[i].astype(F32), m[i], v[i], g))
        return tuple(one[which] for which in range(3) for one in new)

    states, cut = P(("rep", "dp"), None, None), P(None, "dp", None)
    return jax.shard_map(
        step,
        mesh=mesh,
        in_specs=(states, states) + (cut,) * 9,
        out_specs=(P("rep", "dp", None),) * 9,
        check_vma=False,
    )
```

```python
import functools

import jax
import jax.numpy as jnp
from jax import lax
from jax.experimental import pallas as pl
from jax.experimental.pallas import tpu as pltpu
from jax.sharding import PartitionSpec as P


F32, BF16 = jnp.float32, jnp.bfloat16
OVER_X = [(0, 2), (2, 0), (1, 3), (3, 1)]
OVER_CORE = [(0, 1), (1, 0), (2, 3), (3, 2)]
OVER_Y = [(0, 1), (1, 0)]


def normed(h):
    wide = h.astype(F32)
    scale = lax.rsqrt(jnp.mean(wide**2, -1, keepdims=True) + 1e-6)
    return (wide * scale).astype(BF16)


def adamw(w, m, v, g):
    m = 0.9 * m + 0.1 * g
    v = 0.95 * v + 0.05 * g * g
    step = m * lax.rsqrt(v + 1e-8) + 0.1 * w
    return (w - 0.02 * step).astype(BF16), m, v


def others(d):
    x, c = d // 2, d % 2
    return d, 2 * x + 1 - c, 2 * (1 - x) + c, 2 * (1 - x) + 1 - c


def assemble_kernel(number, rows, own, own_c, rx, ry, rx_c, ry_c, out, buf, sem_in, sem_out):
    d, r = lax.axis_index("dp"), lax.axis_index("rep")
    half = rows // 2
    own_i, core_i, x_i, xc_i = others(d)
    at = lambda i, n: pl.ds(pl.multiple_of(i, 16), n)
    moves = [
        (own.at[number], own_i * rows, rows),
        (own_c.at[number], core_i * rows, rows),
        (rx, x_i * rows + r * half, half),
        (ry, x_i * rows + (1 - r) * half, half),
        (rx_c, xc_i * rows + r * half, half),
        (ry_c, xc_i * rows + (1 - r) * half, half),
    ]
    ins = [pltpu.make_async_copy(src, buf.at[at(i, n)], sem_in.at[k]) for k, (src, i, n) in enumerate(moves)]
    outs = [pltpu.make_async_copy(buf.at[at(i, n)], out.at[at(i, n)], sem_out.at[k]) for k, (src, i, n) in enumerate(moves)]
    for one in ins:
        one.start()
    for one, two in zip(ins, outs):
        one.wait()
        two.start()
    for one in outs:
        one.wait()


def assembled(number, own, own_c, rx, ry, rx_c, ry_c):
    _, rows, cols = own.shape
    any_space = pl.BlockSpec(memory_space=pl.ANY)
    return pl.pallas_call(
        functools.partial(assemble_kernel, number, rows),
        out_shape=jax.ShapeDtypeStruct((4 * rows, cols), BF16),
        in_specs=[any_space] * 6,
        out_specs=any_space,
        scratch_shapes=[pltpu.VMEM((4 * rows, cols), BF16), pltpu.SemaphoreType.DMA((6,)), pltpu.SemaphoreType.DMA((6,))],
        compiler_params=pltpu.CompilerParams(vmem_limit_bytes=VMEM),
        cost_estimate=pl.CostEstimate(flops=10**9, bytes_accessed=8 * 4 * rows * cols, transcendentals=0),
        name="assemble",
    )(own, own_c, rx, ry, rx_c, ry_c)


VMEM = 63 << 20


def call(kernel, out_shape, grid, in_specs, out_specs, flops, moved, prefetch=None, scratch=()):
    gs = pltpu.PrefetchScalarGridSpec(
        num_scalar_prefetch=0 if prefetch is None else 1,
        grid=grid,
        in_specs=in_specs,
        out_specs=out_specs,
        scratch_shapes=list(scratch),
    )
    return pl.pallas_call(
        kernel,
        out_shape=out_shape,
        grid_spec=gs,
        compiler_params=pltpu.CompilerParams(vmem_limit_bytes=VMEM),
        cost_estimate=pl.CostEstimate(flops=flops, bytes_accessed=moved, transcendentals=0),
    )


def shaped(shape, kind=BF16):
    return jax.ShapeDtypeStruct(shape, kind)


def resident(shape):
    return pl.BlockSpec(shape, lambda *_: (0,) * len(shape), pipeline_mode=pl.Buffered(1))


def turned_of(a):
    return a.astype(F32).T.astype(BF16)


def norm_kernel(x, a, a_t):
    out = normed(x[...])
    a[...] = out
    a_t[...] = turned_of(out)


def turn_kernel(x, x_t):
    x_t[...] = turned_of(x[...])


def back_norm_kernel(by_a, h, by_h, out, out_t):
    new = by_h[...] + jax.vjp(normed, h[...])[1](by_a[...])[0]
    out[...] = new
    out_t[...] = turned_of(new)


def by_rows(kernel, kinds, *arrays, bm=256):
    m, n = arrays[0].shape
    straight, across = pl.BlockSpec((bm, n), lambda i: (i, 0)), pl.BlockSpec((n, bm), lambda i: (0, i))
    return call(
        kernel, [shaped((n, m) if kind == "t" else (m, n)) for kind in kinds], (m // bm,), [straight] * len(arrays),
        [across if kind == "t" else straight for kind in kinds], 10**9, 2 * m * n * (len(arrays) + len(kinds)),
    )(*arrays)


def gate_up_kernel(number, width, outputs, at, a, *refs):
    sources, outs, (buf, sem) = (refs[:4], refs[4:8]), refs[-2 - outputs : -2], refs[-2:]
    by_gate, by_up, hidden = outs[:3]
    t = pl.program_id(0)
    tile = hidden.shape[1]
    rows = buf.shape[2] // 4
    here = lambda first: pl.ds(pl.multiple_of(first, 128), tile)

    def copies(t):
        slot = lax.rem(t, 2)
        out = []
        for p in range(2):
            own, own_c, rx, rx_c = sources[p]
            cut = [own.at[number, :, here(at[4] * width + t * tile)], own_c.at[number, :, here(at[4] * width + t * tile)]]
            cut += [rx.at[:, here(t * tile)], rx_c.at[:, here(t * tile)]]
            for k, src in enumerate(cut):
                dst = buf.at[slot, p, pl.ds(pl.multiple_of(at[k] * rows, rows), rows)]
                out.append(pltpu.make_async_copy(src, dst, sem.at[slot, p, k]))
        return out

    @pl.when(t == 0)
    def _():
        for one in copies(t):
            one.start()

    @pl.when(t + 1 < pl.num_programs(0))
    def _():
        for one in copies(t + 1):
            one.start()

    for one in copies(t):
        one.wait()
    slot = lax.rem(t, 2)
    for p, whole in enumerate(outs[3:]):
        whole[...] = buf[slot, p]
    g = jnp.dot(a[...], buf[slot, 0], preferred_element_type=F32)
    u = jnp.dot(a[...], buf[slot, 1], preferred_element_type=F32)
    s = jax.nn.sigmoid(g)
    silu = g * s
    by_gate[...] = u * (s + silu * (1 - s))
    by_up[...] = silu
    hidden[...] = (silu * u).astype(BF16)


def gate_up(number, at, a, gates, ups, before=()):
    m, k = a.shape
    n, width = gates[0].shape[2], gates[2].shape[1]
    bn = 256
    tiles = width // bn
    any_space = pl.BlockSpec(memory_space=pl.ANY)
    place = lambda t, at: (0, at[4] * tiles + t)
    out, w = pl.BlockSpec((m, bn), place), pl.BlockSpec((k, bn), place)
    return pl.pallas_call(
        functools.partial(gate_up_kernel, number, width, 5 if number else 3),
        out_shape=[shaped((m, n), F32), shaped((m, n), F32), shaped((m, n))] + [shaped((k, n))] * (2 if number else 0),
        grid_spec=pltpu.PrefetchScalarGridSpec(
            num_scalar_prefetch=1,
            grid=(tiles,),
            in_specs=[resident((m, k))] + [any_space] * (8 + len(before)),
            out_specs=[out] * 3 + [w] * (2 if number else 0),
            scratch_shapes=[pltpu.VMEM((2, 2, k, bn), BF16), pltpu.SemaphoreType.DMA((2, 2, 4))],
        ),
        input_output_aliases={10 + i: i for i in range(len(before))},
        compiler_params=pltpu.CompilerParams(vmem_limit_bytes=VMEM),
        cost_estimate=pl.CostEstimate(flops=4 * m * width * k, bytes_accessed=10 * m * width + 4 * k * width, transcendentals=0),
        name="gate_up",
    )(at, a, *gates, *ups, *before)


def down_kernel(hidden, w, x, h, a, a_t):
    out = x[...] + jnp.dot(hidden[...], w[...], preferred_element_type=F32).astype(BF16)
    h[...] = out
    out = normed(out)
    a[...] = out
    a_t[...] = turned_of(out)


def down(hidden, w, x, bm=256):
    m, k = hidden.shape
    n = w.shape[1]
    out = pl.BlockSpec((bm, n), lambda i: (i, 0))
    return call(
        down_kernel, [shaped((m, n))] * 2 + [shaped((n, m))], (m // bm,),
        [pl.BlockSpec((bm, k), lambda i: (i, 0)), resident((k, n)), out], [out] * 2 + [pl.BlockSpec((n, bm), lambda i: (0, i))],
        2 * m * n * k, 2 * k * n + 2 * m * k,
    )(hidden, w, x)


NT = (((1,), (1,)), ((), ()))


def by_hidden_kernel(dy, w, gate, up, dg, du):
    by = lax.dot_general(dy[...], w[...], NT, preferred_element_type=F32).astype(BF16).astype(F32)
    dg[...] = (by * gate[...]).astype(BF16)
    du[...] = (by * up[...]).astype(BF16)


def by_hidden(dy, w, gate, up, bm=2048, bn=512):
    m, k = dy.shape
    n = w.shape[0]
    out = pl.BlockSpec((bm, bn), lambda j, i: (i, j))
    return call(
        by_hidden_kernel, [shaped((m, n))] * 2, (n // bn, m // bm),
        [resident((m, k)), pl.BlockSpec((bn, k), lambda j, i: (j, 0)), out, out], [out] * 2,
        2 * m * n * k, 12 * m * n,
    )(dy, w, gate, up)


def by_a_kernel(dg, du, wg, wu, out):
    one = lax.dot_general(dg[...], wg[...], NT, preferred_element_type=F32).astype(BF16)
    two = lax.dot_general(du[...], wu[...], NT, preferred_element_type=F32).astype(BF16)
    out[...] = one + two


def by_a(dg, du, wg, wu, bm=1024, bn=512):
    m, k = dg.shape
    n = wg.shape[0]
    lhs = pl.BlockSpec((bm, k), lambda i, j: (i, 0))
    w = pl.BlockSpec((bn, k), lambda i, j: (j, 0))
    return call(
        by_a_kernel, shaped((m, n)), (m // bm, n // bn), [lhs, lhs, w, w], pl.BlockSpec((bm, bn), lambda i, j: (i, j)),
        4 * m * n * k, 4 * m * k + 4 * n * k * (m // bm),
    )(dg, du, wg, wu)


TILE = 512


def exchange(d, src, dst, send_sem, recv_sem):
    return pltpu.make_async_remote_copy(
        src_ref=src, dst_ref=dst, send_sem=send_sem, recv_sem=recv_sem, device_id={"dp": others(d)[1]}, device_id_type=pl.DeviceIdType.MESH
    )


def greet(d):
    barrier = pltpu.get_barrier_semaphore()
    pl.semaphore_signal(barrier, inc=1, device_id={"dp": others(d)[1]}, device_id_type=pl.DeviceIdType.MESH)
    pl.semaphore_wait(barrier, 1)


def term_rows_kernel(left, right, send, kept, three, full, there, send_sem, recv_sem):
    d = lax.axis_index("dp")
    _, core_i, x_i, xc_i = others(d)
    rows, tile = send.shape
    tiles = full.shape[1] // tile
    j = pl.program_id(0)
    cols = lambda k: pl.ds(pl.multiple_of(k * tile, tile), tile)

    def copies(k):
        return [
            exchange(d, full.at[pl.ds(n * rows, rows), cols(k)], there.at[n, :, cols(k)], send_sem.at[n, k], recv_sem.at[n, k])
            for n in range(2)
        ]

    @pl.when(j == 0)
    def _():
        greet(d)
        for n, i in enumerate((core_i, xc_i, x_i)):
            three[pl.ds(n * rows, rows), :] = left[pl.ds(pl.multiple_of(i * rows, rows), rows), :]

    @pl.when((j >= 1) & (j <= tiles))
    def _():
        for one in copies(j - 1):
            one.start()

    @pl.when(j < tiles)
    def _():
        full[:, cols(j)] = jnp.dot(three[...], right[...], preferred_element_type=F32).astype(BF16)

    @pl.when(j >= 2)
    def _():
        k = j - 2
        for one in copies(k):
            one.wait()
        kept[...] = there[0, :, cols(k)]
        send[...] = (full[pl.ds(2 * rows, rows), cols(k)].astype(F32) + there[1, :, cols(k)].astype(F32)).astype(BF16)


def term_rows(left, right):
    m, k = left.shape
    n, rows, tiles = right.shape[1], m // 4, right.shape[1] // TILE
    out = pl.BlockSpec((rows, TILE), lambda j: (0, jnp.maximum(j - 2, 0)))
    return pl.pallas_call(
        term_rows_kernel,
        out_shape=[shaped((rows, n)), shaped((rows, n))],
        grid=(tiles + 2,),
        in_specs=[resident((m, k)), pl.BlockSpec((k, TILE), lambda j: (0, jnp.minimum(j, tiles - 1)))],
        out_specs=[out, out],
        scratch_shapes=[
            pltpu.VMEM((3 * rows, k), BF16),
            pltpu.VMEM((3 * rows, n), BF16),
            pltpu.VMEM((2, rows, n), BF16),
            pltpu.SemaphoreType.DMA((2, tiles)),
            pltpu.SemaphoreType.DMA((2, tiles)),
        ],
        compiler_params=pltpu.CompilerParams(vmem_limit_bytes=VMEM, collective_id=0, has_side_effects=True),
        cost_estimate=pl.CostEstimate(flops=3 * m * n * k // 2, bytes_accessed=2 * (m * k + k * n + m * n), transcendentals=0),
        name="term_rows",
    )(left, right)


def count(squares, g):
    @pl.when(pl.program_id(0) == 0)
    def _():
        squares[0, 0] = 0.0

    squares[0, 0] += jnp.sum(g * g)


def own_rows_kernel(at, left, right, kept, out):
    out[...] = jnp.dot(left[...], right[...], preferred_element_type=F32) + kept[...].astype(F32)


def own_rows_end_kernel(at, left, right, kept, arrived, out, squares):
    total = jnp.dot(left[...], right[...], preferred_element_type=F32) + kept[...].astype(F32)
    g = (total + arrived[...].astype(F32)).astype(BF16)
    out[...] = g
    count(squares, g.astype(F32))


def own_rows(at, left, right, kept, arrived=None):
    m, k = left.shape
    n, rows = right.shape[1], m // 4
    out = pl.BlockSpec((rows, TILE), lambda j, at: (0, j))
    ins = [pl.BlockSpec((rows, k), lambda j, at: (at[0], 0)), pl.BlockSpec((k, TILE), lambda j, at: (0, j)), out]
    if arrived is None:
        return call(own_rows_kernel, shaped((rows, n), F32), (n // TILE,), ins, out, 2 * rows * n * k, 2 * k * n, at)(at, left, right, kept)
    return call(
        own_rows_end_kernel, [shaped((rows, n)), shaped((1, 1), F32)], (n // TILE,), ins + [out],
        [out, pl.BlockSpec(memory_space=pltpu.SMEM)], 2 * rows * n * k, 2 * k * n, at,
    )(at, left, right, kept, arrived)


def ended_kernel(own, arrived, out, squares):
    g = (own[...] + arrived[...].astype(F32)).astype(BF16)
    out[...] = g
    count(squares, g.astype(F32))


def ended(own, arrived):
    m, n = own.shape
    spec = pl.BlockSpec((m, TILE), lambda j: (0, j))
    return call(
        ended_kernel, [shaped((m, n)), shaped((1, 1), F32)], (n // TILE,), [spec, spec], [spec, pl.BlockSpec(memory_space=pltpu.SMEM)],
        4 * m * n, 8 * m * n,
    )(own, arrived)


def term_columns_kernel(left, right, send, own, full, there, send_sem, recv_sem):
    d = lax.axis_index("dp")
    x, c = d // 2, d % 2
    wide = send.shape[1]
    tile = right.shape[1]
    tiles = full.shape[1] // tile
    j = pl.program_id(0)

    def pieces(s):
        first, end = s * wide, (s + 1) * wide
        if s < 3:
            return [(first, wide, (end - 1) // tile)]
        cut = (tiles - 1) * tile
        return [(first, cut - first, (cut - 1) // tile), (cut, end - cut, tiles - 1)]

    def copies(s):
        out = []
        for p, (first, width, last) in enumerate(pieces(s)):
            n = jnp.where(x == s // 2, 0, 1)
            dst = there.at[n, :, pl.ds(first - s * wide, width)]
            out.append((last, exchange(d, full.at[:, pl.ds(first, width)], dst, send_sem.at[s, p], recv_sem.at[s, p])))
        return out

    @pl.when(j == 0)
    def _():
        greet(d)

    for s in range(4):
        for last, one in copies(s):

            @pl.when((j == last + 1) & (c != s % 2))
            def _(one=one):
                one.start()

    @pl.when(j < tiles)
    def _():
        here = pl.ds(pl.multiple_of(j * tile, tile), tile)
        full[:, here] = jnp.dot(left[...], right[...], preferred_element_type=F32).astype(BF16)

    @pl.when(j == tiles + 1)
    def _():
        for s in range(4):
            for last, one in copies(s):

                @pl.when(c != s % 2)
                def _(one=one):
                    one.wait_send()

                @pl.when(c == s % 2)
                def _(one=one):
                    one.wait_recv()

            @pl.when((c == s % 2) & (x == s // 2))
            def _(s=s):
                own[...] = full[:, pl.ds(s * wide, wide)].astype(F32) + there[0].astype(F32)

            @pl.when((c == s % 2) & (x != s // 2))
            def _(s=s):
                send[...] = (full[:, pl.ds(s * wide, wide)].astype(F32) + there[1].astype(F32)).astype(BF16)


def term_columns(left, right):
    m, k = left.shape
    n, wide, tiles = right.shape[1], right.shape[1] // 4, right.shape[1] // TILE
    return pl.pallas_call(
        term_columns_kernel,
        out_shape=[shaped((m, wide)), shaped((m, wide), F32)],
        grid=(tiles + 2,),
        in_specs=[resident((m, k)), pl.BlockSpec((k, TILE), lambda j: (0, jnp.minimum(j, tiles - 1)))],
        out_specs=[pl.BlockSpec((m, wide), lambda j: (0, 0))] * 2,
        scratch_shapes=[pltpu.VMEM((m, n), BF16), pltpu.VMEM((2, m, wide), BF16), pltpu.SemaphoreType.DMA((4, 2)), pltpu.SemaphoreType.DMA((4, 2))],
        compiler_params=pltpu.CompilerParams(vmem_limit_bytes=VMEM, collective_id=1, has_side_effects=True),
        cost_estimate=pl.CostEstimate(flops=2 * m * n * k, bytes_accessed=2 * (m * k + k * n + m * n), transcendentals=0),
        name="term_columns",
    )(left, right)


def turned_kernel(own, arrived, out, squares):
    g = (own[...] + arrived[...].astype(F32)).astype(BF16).astype(F32)
    count(squares, g)
    out[...] = g.T.astype(BF16)


def turned(own, arrived):
    m, n = own.shape
    bn = 128
    spec = pl.BlockSpec((m, bn), lambda j: (0, j))
    g, squares = pl.pallas_call(
        turned_kernel,
        out_shape=[shaped((n, m)), shaped((1, 1), F32)],
        grid=(n // bn,),
        in_specs=[spec, spec],
        out_specs=[pl.BlockSpec((bn, m), lambda j: (j, 0)), pl.BlockSpec(memory_space=pltpu.SMEM)],
        compiler_params=pltpu.CompilerParams(vmem_limit_bytes=VMEM),
        cost_estimate=pl.CostEstimate(flops=4 * m * n, bytes_accessed=8 * m * n, transcendentals=0),
        name="turned",
    )(own, arrived)
    return g, squares


def solution(mesh):
    def step(x, dy, *arrays):
        weights, m, v = (arrays[i : i + 3] for i in (0, 3, 6))
        d, r = lax.axis_index("dp"), lax.axis_index("rep")
        own_i, core_i, x_i, xc_i = others(d)
        layers = weights[0].shape[0]

        from_core = [lax.ppermute(w, "dp", OVER_CORE) for w in weights]

        def across(i, number):
            rows, cols = weights[i].shape[1:]
            if i == 2:
                mine = lax.dynamic_slice(weights[i], (number, r * (rows // 2), 0), (1, rows // 2, cols))[0]
            else:
                mine = lax.dynamic_slice(weights[i], (number, 0, r * (cols // 2)), (1, rows, cols // 2))[0]
            return lax.ppermute(mine, "dp", OVER_X)

        halves = {(i, number): across(i, number) for number in range(layers) for i in range(3)}

        def first(i, number, *behind):
            rx = halves[i, number]
            if behind:
                rx = lax.optimization_barrier((rx, *behind))[0]
            return lax.ppermute(rx, "dp", OVER_CORE)

        def second(i, number, *behind):
            rx = halves[i, number]
            if behind:
                rx = lax.optimization_barrier((rx, *behind))[0]
            ry = lax.ppermute(rx, "rep", OVER_Y)
            return ry, lax.ppermute(ry, "dp", OVER_CORE)

        def whole_down(number, behind):
            ry, ry_c = second(2, number, behind)
            return assembled(number, weights[2], from_core[2], halves[2, number], ry, first(2, number), ry_c)

        last = []

        def ordered(*some):
            out = lax.optimization_barrier((*some, *last))[: len(some)] if last else some
            return out[0] if len(some) == 1 else out

        def noted(one):
            last[:] = [one]
            return one

        at = jnp.stack([own_i, core_i, x_i, xc_i, r]).astype(jnp.int32)
        at_b = jnp.stack([own_i, core_i, x_i, xc_i, 1 - r]).astype(jnp.int32)

        def ab(number, a, behind):
            arrived = [(weights[i], from_core[i], halves[i, number], first(i, number, *behind[i])) for i in (0, 1)]
            outs = gate_up(number, at, a, *arrived)
            return outs, [(weights[i], from_core[i], *second(i, number, *behind[i])) for i in (0, 1)]

        a0, a0_t = by_rows(norm_kernel, " t", x[0])
        (dy_t,) = by_rows(turn_kernel, "t", lax.optimization_barrier((dy[0], a0, halves[0, 0]))[0])
        a0, a0_t, dy_t = lax.optimization_barrier((a0, a0_t, dy_t))
        outs, arrived = ab(0, a0, ((), ()))
        w_down0 = whole_down(0, outs[2])
        gate0, up0, hidden0 = gate_up(0, at_b, a0, *arrived, outs)
        h1, a1, a1_t = down(hidden0, w_down0, x[0])
        outs, arrived = ab(1, a1, ((hidden0,), (h1,)))
        w_down1 = whole_down(1, outs[2])
        gate1, up1, hidden1, w_gate1, w_up1 = gate_up(1, at_b, a1, *arrived, outs)
        noted(hidden1)

        mine, late = [[None] * 3 for _ in range(layers)], {}

        def term(i, number, kernel, left, right):
            send, kept = kernel(left, ordered(right))
            noted(send)
            late[i, number] = lax.ppermute(send, "dp", OVER_X), kept, left, right

        term(2, 1, term_columns, dy_t, hidden1)
        by_gate, by_up = by_hidden(ordered(dy[0]), w_down1, gate1, up1)
        noted(by_gate)
        term(0, 1, term_rows, a1_t, by_gate)
        term(1, 1, term_rows, a1_t, by_up)
        by_in = by_a(ordered(by_gate), by_up, w_gate1, w_up1)
        by_h, by_h_t = by_rows(back_norm_kernel, " t", by_in, h1, dy[0])
        noted(by_h)
        term(2, 0, term_columns, by_h_t, hidden0)
        by_gate, by_up = by_hidden(ordered(by_h), w_down0, gate0, up0)
        noted(by_gate)
        term(0, 0, term_rows, a0_t, by_gate)
        term(1, 0, term_rows, a0_t, by_up)
        _, kept, left, right = late[1, 0]
        last_own = noted(own_rows(at, left, ordered(right), kept))
        squares = 0.0
        for i, number in ((0, 1), (1, 1), (2, 1), (2, 0), (0, 0), (1, 0)):
            from_x, kept, left, right = late[i, number]
            if i == 2:
                g, more = turned(ordered(kept), from_x)
            elif (i, number) == (1, 0):
                g, more = ended(ordered(last_own), from_x)
            else:
                g, more = own_rows(at, left, ordered(right), kept, from_x)
            mine[number][i] = noted(g)
            squares += more[0, 0]

        squares = lax.psum(squares, "dp")
        count = 4 * sum(g.size for gs in mine for g in gs)
        factor = jnp.minimum(1.0, 0.5 * lax.rsqrt(squares / count + 1e-30))
        new = []
        for i in range(3):
            g = jnp.stack([mine[number][i] for number in range(layers)]).astype(F32) * factor
            new.append(adamw(weights[i].astype(F32), m[i], v[i], g))
        return tuple(one[which] for which in range(3) for one in new)

    states, cut = P(("rep", "dp"), None, None), P(None, "dp", None)
    return jax.shard_map(
        step,
        mesh=mesh,
        in_specs=(states, states) + (cut,) * 9,
        out_specs=(P("rep", "dp", None),) * 9,
        check_vma=False,
    )
```

```python
import functools

import jax
import jax.numpy as jnp
from jax import lax
from jax.experimental import pallas as pl
from jax.experimental.pallas import tpu as pltpu
from jax.sharding import PartitionSpec as P


F32, BF16 = jnp.float32, jnp.bfloat16
OVER_X = [(0, 2), (2, 0), (1, 3), (3, 1)]
OVER_CORE = [(0, 1), (1, 0), (2, 3), (3, 2)]
OVER_Y = [(0, 1), (1, 0)]


def normed(h):
    wide = h.astype(F32)
    scale = lax.rsqrt(jnp.mean(wide**2, -1, keepdims=True) + 1e-6)
    return (wide * scale).astype(BF16)


def adamw(w, m, v, g):
    m = 0.9 * m + 0.1 * g
    v = 0.95 * v + 0.05 * g * g
    step = m * lax.rsqrt(v + 1e-8) + 0.1 * w
    return (w - 0.02 * step).astype(BF16), m, v


def others(d):
    x, c = d // 2, d % 2
    return d, 2 * x + 1 - c, 2 * (1 - x) + c, 2 * (1 - x) + 1 - c


VMEM = 63 << 20


def call(kernel, out_shape, grid, in_specs, out_specs, flops, moved, prefetch=None, scratch=()):
    gs = pltpu.PrefetchScalarGridSpec(
        num_scalar_prefetch=0 if prefetch is None else 1,
        grid=grid,
        in_specs=in_specs,
        out_specs=out_specs,
        scratch_shapes=list(scratch),
    )
    return pl.pallas_call(
        kernel,
        out_shape=out_shape,
        grid_spec=gs,
        compiler_params=pltpu.CompilerParams(vmem_limit_bytes=VMEM),
        cost_estimate=pl.CostEstimate(flops=flops, bytes_accessed=moved, transcendentals=0),
    )


def shaped(shape, kind=BF16):
    return jax.ShapeDtypeStruct(shape, kind)


def resident(shape):
    return pl.BlockSpec(shape, lambda *_: (0,) * len(shape), pipeline_mode=pl.Buffered(1))


def turned_of(a):
    return a.astype(F32).T.astype(BF16)


def norm_kernel(x, a, a_t):
    out = normed(x[...])
    a[...] = out
    a_t[...] = turned_of(out)


def turn_kernel(x, x_t):
    x_t[...] = turned_of(x[...])


def back_norm_kernel(by_a, h, by_h, out, out_t):
    new = by_h[...] + jax.vjp(normed, h[...])[1](by_a[...])[0]
    out[...] = new
    out_t[...] = turned_of(new)


def by_rows(kernel, kinds, *arrays, bm=256):
    m, n = arrays[0].shape
    straight, across = pl.BlockSpec((bm, n), lambda i: (i, 0)), pl.BlockSpec((n, bm), lambda i: (0, i))
    return call(
        kernel, [shaped((n, m) if kind == "t" else (m, n)) for kind in kinds], (m // bm,), [straight] * len(arrays),
        [across if kind == "t" else straight for kind in kinds], 10**9, 2 * m * n * (len(arrays) + len(kinds)),
    )(*arrays)


def gate_up_kernel(number, width, outputs, at, a, *refs):
    sources, outs, (buf, sem) = (refs[:4], refs[4:8]), refs[-2 - outputs : -2], refs[-2:]
    by_gate, by_up, hidden = outs[:3]
    t = pl.program_id(0)
    tile = hidden.shape[1]
    rows = buf.shape[2] // 4
    here = lambda first: pl.ds(pl.multiple_of(first, 128), tile)

    def copies(t):
        slot = lax.rem(t, 2)
        out = []
        for p in range(2):
            own, own_c, rx, rx_c = sources[p]
            cut = [own.at[number, :, here(at[4] * width + t * tile)], own_c.at[number, :, here(at[4] * width + t * tile)]]
            cut += [rx.at[:, here(t * tile)], rx_c.at[:, here(t * tile)]]
            for k, src in enumerate(cut):
                dst = buf.at[slot, p, pl.ds(pl.multiple_of(at[k] * rows, rows), rows)]
                out.append(pltpu.make_async_copy(src, dst, sem.at[slot, p, k]))
        return out

    @pl.when(t == 0)
    def _():
        for one in copies(t):
            one.start()

    @pl.when(t + 1 < pl.num_programs(0))
    def _():
        for one in copies(t + 1):
            one.start()

    for one in copies(t):
        one.wait()
    slot = lax.rem(t, 2)
    for p, whole in enumerate(outs[3:]):
        whole[...] = buf[slot, p]
    g = jnp.dot(a[...], buf[slot, 0], preferred_element_type=F32)
    u = jnp.dot(a[...], buf[slot, 1], preferred_element_type=F32)
    s = jax.nn.sigmoid(g)
    silu = g * s
    by_gate[...] = u * (s + silu * (1 - s))
    by_up[...] = silu
    hidden[...] = (silu * u).astype(BF16)


def gate_up(number, at, a, gates, ups, before=()):
    m, k = a.shape
    n, width = gates[0].shape[2], gates[2].shape[1]
    bn = 256
    tiles = width // bn
    any_space = pl.BlockSpec(memory_space=pl.ANY)
    place = lambda t, at: (0, at[4] * tiles + t)
    out, w = pl.BlockSpec((m, bn), place), pl.BlockSpec((k, bn), place)
    return pl.pallas_call(
        functools.partial(gate_up_kernel, number, width, 5 if number else 3),
        out_shape=[shaped((m, n), F32), shaped((m, n), F32), shaped((m, n))] + [shaped((k, n))] * (2 if number else 0),
        grid_spec=pltpu.PrefetchScalarGridSpec(
            num_scalar_prefetch=1,
            grid=(tiles,),
            in_specs=[resident((m, k))] + [any_space] * (8 + len(before)),
            out_specs=[out] * 3 + [w] * (2 if number else 0),
            scratch_shapes=[pltpu.VMEM((2, 2, k, bn), BF16), pltpu.SemaphoreType.DMA((2, 2, 4))],
        ),
        input_output_aliases={10 + i: i for i in range(len(before))},
        compiler_params=pltpu.CompilerParams(vmem_limit_bytes=VMEM),
        cost_estimate=pl.CostEstimate(flops=4 * m * width * k, bytes_accessed=10 * m * width + 4 * k * width, transcendentals=0),
        name="gate_up",
    )(at, a, *gates, *ups, *before)


def arriving(number, rows, pieces, buf, sem):
    own, own_c, rx, ry, rx_c, ry_c = pieces
    d, r = lax.axis_index("dp"), lax.axis_index("rep")
    half = rows // 2
    own_i, core_i, x_i, xc_i = others(d)
    at = lambda i, n: buf.at[pl.ds(pl.multiple_of(i, 16), n)]
    moves = [
        (own.at[number], at(own_i * rows, rows)),
        (own_c.at[number], at(core_i * rows, rows)),
        (rx, at(x_i * rows + r * half, half)),
        (ry, at(x_i * rows + (1 - r) * half, half)),
        (rx_c, at(xc_i * rows + r * half, half)),
        (ry_c, at(xc_i * rows + (1 - r) * half, half)),
    ]
    return [pltpu.make_async_copy(src, dst, sem.at[k]) for k, (src, dst) in enumerate(moves)]


def down_kernel(number, rows, hidden, x, *refs):
    pieces, (h, a, a_t, whole, buf, sem, out_sem) = refs[:6], refs[6:]
    i = pl.program_id(0)
    put = pltpu.make_async_copy(buf, whole, out_sem)

    @pl.when(i == 0)
    def _():
        ins = arriving(number, rows, pieces, buf, sem)
        for one in ins:
            one.start()
        for one in ins:
            one.wait()
        put.start()

    out = x[...] + jnp.dot(hidden[...], buf[...], preferred_element_type=F32).astype(BF16)
    h[...] = out
    out = normed(out)
    a[...] = out
    a_t[...] = turned_of(out)

    @pl.when(i == pl.num_programs(0) - 1)
    def _():
        put.wait()


def down(number, hidden, x, pieces, bm=256):
    m, k = hidden.shape
    n, rows = pieces[0].shape[2], pieces[0].shape[1]
    out = pl.BlockSpec((bm, n), lambda i: (i, 0))
    any_space = pl.BlockSpec(memory_space=pl.ANY)
    return call(
        functools.partial(down_kernel, number, rows), [shaped((m, n))] * 2 + [shaped((n, m)), shaped((k, n))], (m // bm,),
        [pl.BlockSpec((bm, k), lambda i: (i, 0)), out] + [any_space] * 6,
        [out] * 2 + [pl.BlockSpec((n, bm), lambda i: (0, i)), any_space], 2 * m * n * k, 4 * k * n + 2 * m * k,
        scratch=[pltpu.VMEM((k, n), BF16), pltpu.SemaphoreType.DMA((6,)), pltpu.SemaphoreType.DMA],
    )(hidden, x, *pieces)


NT = (((1,), (1,)), ((), ()))


def by_hidden_kernel(dy, w, gate, up, dg, du):
    by = lax.dot_general(dy[...], w[...], NT, preferred_element_type=F32).astype(BF16).astype(F32)
    dg[...] = (by * gate[...]).astype(BF16)
    du[...] = (by * up[...]).astype(BF16)


def by_hidden(dy, w, gate, up, bn=512):
    m, k = dy.shape
    n = w.shape[0]
    out = pl.BlockSpec((m, bn), lambda j: (0, j))
    return call(
        by_hidden_kernel, [shaped((m, n))] * 2, (n // bn,),
        [resident((m, k)), pl.BlockSpec((bn, k), lambda j: (j, 0)), out, out], [out] * 2, 2 * m * n * k, 12 * m * n,
    )(dy, w, gate, up)


def by_hidden_pieces_kernel(number, rows, dy, gate, up, *refs):
    pieces, (dg, du, buf, sem) = refs[:6], refs[6:]
    j, bn = pl.program_id(0), dg.shape[1]

    @pl.when(j == 0)
    def _():
        ins = arriving(number, rows, pieces, buf, sem)
        for one in ins:
            one.start()
        for one in ins:
            one.wait()

    w = buf[pl.ds(pl.multiple_of(j * bn, bn), bn), :]
    by = lax.dot_general(dy[...], w, NT, preferred_element_type=F32).astype(BF16).astype(F32)
    dg[...] = (by * gate[...]).astype(BF16)
    du[...] = (by * up[...]).astype(BF16)


def by_hidden_pieces(number, dy, pieces, gate, up, bn=512):
    m, k = dy.shape
    n, rows = gate.shape[1], pieces[0].shape[1]
    out = pl.BlockSpec((m, bn), lambda j: (0, j))
    return call(
        functools.partial(by_hidden_pieces_kernel, number, rows), [shaped((m, n))] * 2, (n // bn,),
        [resident((m, k)), out, out] + [pl.BlockSpec(memory_space=pl.ANY)] * 6, [out] * 2, 2 * m * n * k, 12 * m * n,
        scratch=[pltpu.VMEM((n, k), BF16), pltpu.SemaphoreType.DMA((6,))],
    )(dy, gate, up, *pieces)


def by_a_kernel(dg, du, wg, wu, out):
    one = lax.dot_general(dg[...], wg[...], NT, preferred_element_type=F32).astype(BF16)
    two = lax.dot_general(du[...], wu[...], NT, preferred_element_type=F32).astype(BF16)
    out[...] = one + two


def by_a(dg, du, wg, wu, bm=1024, bn=512):
    m, k = dg.shape
    n = wg.shape[0]
    lhs = pl.BlockSpec((bm, k), lambda i, j: (i, 0))
    w = pl.BlockSpec((bn, k), lambda i, j: (j, 0))
    return call(
        by_a_kernel, shaped((m, n)), (m // bm, n // bn), [lhs, lhs, w, w], pl.BlockSpec((bm, bn), lambda i, j: (i, j)),
        4 * m * n * k, 4 * m * k + 4 * n * k * (m // bm),
    )(dg, du, wg, wu)


TILE = 512


def exchange(d, src, dst, send_sem, recv_sem):
    return pltpu.make_async_remote_copy(
        src_ref=src, dst_ref=dst, send_sem=send_sem, recv_sem=recv_sem, device_id={"dp": others(d)[1]}, device_id_type=pl.DeviceIdType.MESH
    )


def greet(d):
    barrier = pltpu.get_barrier_semaphore()
    pl.semaphore_signal(barrier, inc=1, device_id={"dp": others(d)[1]}, device_id_type=pl.DeviceIdType.MESH)
    pl.semaphore_wait(barrier, 1)


def term_rows_kernel(left, right, send, kept, three, full, there, send_sem, recv_sem):
    d = lax.axis_index("dp")
    _, core_i, x_i, xc_i = others(d)
    rows, tile = send.shape
    tiles = full.shape[1] // tile
    j = pl.program_id(0)
    cols = lambda k: pl.ds(pl.multiple_of(k * tile, tile), tile)

    def copies(k):
        return [
            exchange(d, full.at[pl.ds(n * rows, rows), cols(k)], there.at[n, :, cols(k)], send_sem.at[n, k], recv_sem.at[n, k])
            for n in range(2)
        ]

    @pl.when(j == 0)
    def _():
        greet(d)
        for n, i in enumerate((core_i, xc_i, x_i)):
            three[pl.ds(n * rows, rows), :] = left[pl.ds(pl.multiple_of(i * rows, rows), rows), :]

    @pl.when((j >= 1) & (j <= tiles))
    def _():
        for one in copies(j - 1):
            one.start()

    @pl.when(j < tiles)
    def _():
        full[:, cols(j)] = jnp.dot(three[...], right[...], preferred_element_type=F32).astype(BF16)

    @pl.when(j >= 2)
    def _():
        k = j - 2
        for one in copies(k):
            one.wait()
        kept[...] = there[0, :, cols(k)]
        send[...] = (full[pl.ds(2 * rows, rows), cols(k)].astype(F32) + there[1, :, cols(k)].astype(F32)).astype(BF16)


def term_rows(left, right):
    m, k = left.shape
    n, rows, tiles = right.shape[1], m // 4, right.shape[1] // TILE
    out = pl.BlockSpec((rows, TILE), lambda j: (0, jnp.maximum(j - 2, 0)))
    return pl.pallas_call(
        term_rows_kernel,
        out_shape=[shaped((rows, n)), shaped((rows, n))],
        grid=(tiles + 2,),
        in_specs=[resident((m, k)), pl.BlockSpec((k, TILE), lambda j: (0, jnp.minimum(j, tiles - 1)))],
        out_specs=[out, out],
        scratch_shapes=[
            pltpu.VMEM((3 * rows, k), BF16),
            pltpu.VMEM((3 * rows, n), BF16),
            pltpu.VMEM((2, rows, n), BF16),
            pltpu.SemaphoreType.DMA((2, tiles)),
            pltpu.SemaphoreType.DMA((2, tiles)),
        ],
        compiler_params=pltpu.CompilerParams(vmem_limit_bytes=VMEM, collective_id=0, has_side_effects=True),
        cost_estimate=pl.CostEstimate(flops=3 * m * n * k // 2, bytes_accessed=2 * (m * k + k * n + m * n), transcendentals=0),
        name="term_rows",
    )(left, right)


def count(squares, g):
    @pl.when(pl.program_id(0) == 0)
    def _():
        squares[0, 0] = 0.0

    squares[0, 0] += jnp.sum(g * g)


def own_rows_kernel(at, left, right, kept, out):
    out[...] = jnp.dot(left[...], right[...], preferred_element_type=F32) + kept[...].astype(F32)


def own_rows_end_kernel(at, left, right, kept, arrived, out, squares):
    total = jnp.dot(left[...], right[...], preferred_element_type=F32) + kept[...].astype(F32)
    g = (total + arrived[...].astype(F32)).astype(BF16)
    out[...] = g
    count(squares, g.astype(F32))


def own_rows(at, left, right, kept, arrived=None):
    m, k = left.shape
    n, rows = right.shape[1], m // 4
    out = pl.BlockSpec((rows, TILE), lambda j, at: (0, j))
    ins = [pl.BlockSpec((rows, k), lambda j, at: (at[0], 0)), pl.BlockSpec((k, TILE), lambda j, at: (0, j)), out]
    if arrived is None:
        return call(own_rows_kernel, shaped((rows, n), F32), (n // TILE,), ins, out, 2 * rows * n * k, 2 * k * n, at)(at, left, right, kept)
    return call(
        own_rows_end_kernel, [shaped((rows, n)), shaped((1, 1), F32)], (n // TILE,), ins + [out],
        [out, pl.BlockSpec(memory_space=pltpu.SMEM)], 2 * rows * n * k, 2 * k * n, at,
    )(at, left, right, kept, arrived)


def ended_kernel(elements, own, arrived, before, out, factor, acc, mine, got, send_sem, recv_sem):
    d = lax.axis_index("dp")
    j, last = pl.program_id(0), pl.num_programs(0) - 1
    peers = [lax.rem(d + k, 4) for k in (1, 2, 3)]
    barrier = pltpu.get_barrier_semaphore()

    @pl.when(j == 0)
    def _():
        for peer in peers:
            pl.semaphore_signal(barrier, inc=1, device_id={"dp": peer}, device_id_type=pl.DeviceIdType.MESH)
        acc[...] = jnp.zeros_like(acc)

    g = (own[...] + arrived[...].astype(F32)).astype(BF16)
    out[...] = g
    g = g.astype(F32)
    acc[...] += jnp.sum((g * g).reshape(g.shape[0] // 8, 8, g.shape[1]), axis=0)

    @pl.when(j == last)
    def _():
        mine[...] = jnp.full(mine.shape, jnp.sum(acc[...]) + before[0, 0], F32)
        pl.semaphore_wait(barrier, 3)
        copies = [
            pltpu.make_async_remote_copy(
                src_ref=mine, dst_ref=got.at[k], send_sem=send_sem.at[k], recv_sem=recv_sem.at[k],
                device_id={"dp": peer}, device_id_type=pl.DeviceIdType.MESH,
            )
            for k, peer in enumerate(peers)
        ]
        for one in copies:
            one.start()
        for one in copies:
            one.wait()
        squares = mine[...] + got[0] + got[1] + got[2]
        factor[...] = jnp.minimum(1.0, 0.5 * lax.rsqrt(squares / elements + 1e-30))


def ended(own, arrived, before, elements):
    m, n = own.shape
    spec = pl.BlockSpec((m, TILE), lambda j: (0, j))
    return pl.pallas_call(
        functools.partial(ended_kernel, elements),
        out_shape=[shaped((m, n)), shaped((8, 128), F32)],
        grid=(n // TILE,),
        in_specs=[spec, spec, pl.BlockSpec(memory_space=pltpu.SMEM)],
        out_specs=[spec, pl.BlockSpec((8, 128), lambda j: (0, 0))],
        scratch_shapes=[
            pltpu.VMEM((8, TILE), F32),
            pltpu.VMEM((8, 128), F32),
            pltpu.VMEM((3, 8, 128), F32),
            pltpu.SemaphoreType.DMA((3,)),
            pltpu.SemaphoreType.DMA((3,)),
        ],
        compiler_params=pltpu.CompilerParams(vmem_limit_bytes=VMEM, collective_id=2, has_side_effects=True),
        cost_estimate=pl.CostEstimate(flops=4 * m * n, bytes_accessed=8 * m * n, transcendentals=0),
        name="ended",
    )(own, arrived, before)


def term_columns_kernel(left, right, send, own, full, there, send_sem, recv_sem):
    d = lax.axis_index("dp")
    x, c = d // 2, d % 2
    wide = send.shape[1]
    tile = right.shape[1]
    tiles = full.shape[1] // tile
    j = pl.program_id(0)

    def pieces(s):
        first, end = s * wide, (s + 1) * wide
        if s < 3:
            return [(first, wide, (end - 1) // tile)]
        cut = (tiles - 1) * tile
        return [(first, cut - first, (cut - 1) // tile), (cut, end - cut, tiles - 1)]

    def copies(s):
        out = []
        for p, (first, width, last) in enumerate(pieces(s)):
            n = jnp.where(x == s // 2, 0, 1)
            dst = there.at[n, :, pl.ds(first - s * wide, width)]
            out.append((last, exchange(d, full.at[:, pl.ds(first, width)], dst, send_sem.at[s, p], recv_sem.at[s, p])))
        return out

    @pl.when(j == 0)
    def _():
        greet(d)

    for s in range(4):
        for last, one in copies(s):

            @pl.when((j == last + 1) & (c != s % 2))
            def _(one=one):
                one.start()

    @pl.when(j < tiles)
    def _():
        here = pl.ds(pl.multiple_of(j * tile, tile), tile)
        full[:, here] = jnp.dot(left[...], right[...], preferred_element_type=F32).astype(BF16)

    @pl.when(j == tiles + 1)
    def _():
        for s in range(4):
            for last, one in copies(s):

                @pl.when(c != s % 2)
                def _(one=one):
                    one.wait_send()

                @pl.when(c == s % 2)
                def _(one=one):
                    one.wait_recv()

            @pl.when((c == s % 2) & (x == s // 2))
            def _(s=s):
                own[...] = full[:, pl.ds(s * wide, wide)].astype(F32) + there[0].astype(F32)

            @pl.when((c == s % 2) & (x != s // 2))
            def _(s=s):
                send[...] = (full[:, pl.ds(s * wide, wide)].astype(F32) + there[1].astype(F32)).astype(BF16)


def term_columns(left, right):
    m, k = left.shape
    n, wide, tiles = right.shape[1], right.shape[1] // 4, right.shape[1] // TILE
    return pl.pallas_call(
        term_columns_kernel,
        out_shape=[shaped((m, wide)), shaped((m, wide), F32)],
        grid=(tiles + 2,),
        in_specs=[resident((m, k)), pl.BlockSpec((k, TILE), lambda j: (0, jnp.minimum(j, tiles - 1)))],
        out_specs=[pl.BlockSpec((m, wide), lambda j: (0, 0))] * 2,
        scratch_shapes=[pltpu.VMEM((m, n), BF16), pltpu.VMEM((2, m, wide), BF16), pltpu.SemaphoreType.DMA((4, 2)), pltpu.SemaphoreType.DMA((4, 2))],
        compiler_params=pltpu.CompilerParams(vmem_limit_bytes=VMEM, collective_id=1, has_side_effects=True),
        cost_estimate=pl.CostEstimate(flops=2 * m * n * k, bytes_accessed=2 * (m * k + k * n + m * n), transcendentals=0),
        name="term_columns",
    )(left, right)


def turned_kernel(own, arrived, out, squares):
    g = (own[...] + arrived[...].astype(F32)).astype(BF16).astype(F32)
    count(squares, g)
    out[...] = g.T.astype(BF16)


def turned(own, arrived):
    m, n = own.shape
    bn = 128
    spec = pl.BlockSpec((m, bn), lambda j: (0, j))
    g, squares = pl.pallas_call(
        turned_kernel,
        out_shape=[shaped((n, m)), shaped((1, 1), F32)],
        grid=(n // bn,),
        in_specs=[spec, spec],
        out_specs=[pl.BlockSpec((bn, m), lambda j: (j, 0)), pl.BlockSpec(memory_space=pltpu.SMEM)],
        compiler_params=pltpu.CompilerParams(vmem_limit_bytes=VMEM),
        cost_estimate=pl.CostEstimate(flops=4 * m * n, bytes_accessed=8 * m * n, transcendentals=0),
        name="turned",
    )(own, arrived)
    return g, squares


def solution(mesh):
    def step(x, dy, *arrays):
        weights, m, v = (arrays[i : i + 3] for i in (0, 3, 6))
        d, r = lax.axis_index("dp"), lax.axis_index("rep")
        own_i, core_i, x_i, xc_i = others(d)
        layers = weights[0].shape[0]

        from_core = [lax.ppermute(w, "dp", OVER_CORE) for w in weights]

        def across(i, number):
            rows, cols = weights[i].shape[1:]
            if i == 2:
                mine = lax.dynamic_slice(weights[i], (number, r * (rows // 2), 0), (1, rows // 2, cols))[0]
            else:
                mine = lax.dynamic_slice(weights[i], (number, 0, r * (cols // 2)), (1, rows, cols // 2))[0]
            return lax.ppermute(mine, "dp", OVER_X)

        halves = {(i, number): across(i, number) for number in range(layers) for i in range(3)}

        def first(i, number, *behind):
            rx = halves[i, number]
            if behind:
                rx = lax.optimization_barrier((rx, *behind))[0]
            return lax.ppermute(rx, "dp", OVER_CORE)

        def second(i, number, *behind):
            rx = halves[i, number]
            if behind:
                rx = lax.optimization_barrier((rx, *behind))[0]
            ry = lax.ppermute(rx, "rep", OVER_Y)
            return ry, lax.ppermute(ry, "dp", OVER_CORE)

        def down_pieces(number, behind):
            ry, ry_c = second(2, number, behind)
            return weights[2], from_core[2], halves[2, number], ry, first(2, number), ry_c

        last = []

        def ordered(*some):
            out = lax.optimization_barrier((*some, *last))[: len(some)] if last else some
            return out[0] if len(some) == 1 else out

        def noted(one):
            last[:] = [one]
            return one

        at = jnp.stack([own_i, core_i, x_i, xc_i, r]).astype(jnp.int32)
        at_b = jnp.stack([own_i, core_i, x_i, xc_i, 1 - r]).astype(jnp.int32)

        def ab(number, a, behind):
            arrived = [(weights[i], from_core[i], halves[i, number], first(i, number, *behind[i])) for i in (0, 1)]
            outs = gate_up(number, at, a, *arrived)
            return outs, [(weights[i], from_core[i], *second(i, number, *behind[i])) for i in (0, 1)]

        a0, a0_t = by_rows(norm_kernel, " t", x[0])
        (dy_t,) = by_rows(turn_kernel, "t", lax.optimization_barrier((dy[0], a0, halves[0, 0]))[0])
        a0, a0_t, dy_t = lax.optimization_barrier((a0, a0_t, dy_t))
        outs, arrived = ab(0, a0, ((), ()))
        pieces0 = down_pieces(0, outs[2])
        gate0, up0, hidden0 = gate_up(0, at_b, a0, *arrived, outs)
        h1, a1, a1_t, w_down0 = down(0, hidden0, x[0], pieces0)
        outs, arrived = ab(1, a1, ((hidden0,), (h1,)))
        pieces1 = down_pieces(1, outs[2])
        gate1, up1, hidden1, w_gate1, w_up1 = gate_up(1, at_b, a1, *arrived, outs)
        noted(hidden1)

        mine, late = [[None] * 3 for _ in range(layers)], {}

        def term(i, number, kernel, left, right):
            send, kept = kernel(left, ordered(right))
            noted(send)
            late[i, number] = lax.ppermute(send, "dp", OVER_X), kept, left, right

        term(2, 1, term_columns, dy_t, hidden1)
        by_gate, by_up = by_hidden_pieces(1, ordered(dy[0]), pieces1, gate1, up1)
        noted(by_gate)
        term(0, 1, term_rows, a1_t, by_gate)
        term(1, 1, term_rows, a1_t, by_up)
        by_in = by_a(ordered(by_gate), by_up, w_gate1, w_up1)
        by_h, by_h_t = by_rows(back_norm_kernel, " t", by_in, h1, dy[0])
        noted(by_h)
        term(2, 0, term_columns, by_h_t, hidden0)
        by_gate, by_up = by_hidden(ordered(by_h), w_down0, gate0, up0)
        noted(by_gate)
        term(0, 0, term_rows, a0_t, by_gate)
        term(1, 0, term_rows, a0_t, by_up)
        _, kept, left, right = late[1, 0]
        last_own = noted(own_rows(at, left, ordered(right), kept))
        squares = 0.0
        for i, number in ((0, 1), (1, 1), (2, 1), (2, 0), (0, 0)):
            from_x, kept, left, right = late[i, number]
            if i == 2:
                g, more = turned(ordered(kept), from_x)
            else:
                g, more = own_rows(at, left, ordered(right), kept, from_x)
            mine[number][i] = noted(g)
            squares += more
        count = 4 * sum(w.size for w in weights)
        mine[0][1], factor = ended(ordered(last_own), late[1, 0][0], squares, count)
        factor = factor[0, 0]
        new = []
        for i in range(3):
            g = jnp.stack([mine[number][i] for number in range(layers)]).astype(F32) * factor
            new.append(adamw(weights[i].astype(F32), m[i], v[i], g))
        return tuple(one[which] for which in range(3) for one in new)

    states, cut = P(("rep", "dp"), None, None), P(None, "dp", None)
    return jax.shard_map(
        step,
        mesh=mesh,
        in_specs=(states, states) + (cut,) * 9,
        out_specs=(P("rep", "dp", None),) * 9,
        check_vma=False,
    )
```

```python
import functools

import jax
import jax.numpy as jnp
from jax import lax
from jax.experimental import pallas as pl
from jax.experimental.pallas import tpu as pltpu
from jax.sharding import PartitionSpec as P


F32, BF16 = jnp.float32, jnp.bfloat16
OVER_X = [(0, 2), (2, 0), (1, 3), (3, 1)]
OVER_CORE = [(0, 1), (1, 0), (2, 3), (3, 2)]
OVER_Y = [(0, 1), (1, 0)]


def normed(h):
    wide = h.astype(F32)
    scale = lax.rsqrt(jnp.mean(wide**2, -1, keepdims=True) + 1e-6)
    return (wide * scale).astype(BF16)


def adamw(w, m, v, g):
    m = 0.9 * m + 0.1 * g
    v = 0.95 * v + 0.05 * g * g
    step = m * lax.rsqrt(v + 1e-8) + 0.1 * w
    return (w - 0.02 * step).astype(BF16), m, v


def others(d):
    x, c = d // 2, d % 2
    return d, 2 * x + 1 - c, 2 * (1 - x) + c, 2 * (1 - x) + 1 - c


VMEM = 63 << 20
FREE = 0


def call(kernel, out_shape, grid, in_specs, out_specs, flops, moved, prefetch=None, scratch=()):
    gs = pltpu.PrefetchScalarGridSpec(
        num_scalar_prefetch=0 if prefetch is None else 1,
        grid=grid,
        in_specs=in_specs,
        out_specs=out_specs,
        scratch_shapes=list(scratch),
    )
    return pl.pallas_call(
        kernel,
        out_shape=out_shape,
        grid_spec=gs,
        compiler_params=pltpu.CompilerParams(vmem_limit_bytes=VMEM),
        cost_estimate=pl.CostEstimate(flops=flops, bytes_accessed=moved, transcendentals=FREE),
    )


def shaped(shape, kind=BF16):
    return jax.ShapeDtypeStruct(shape, kind)


def resident(shape):
    return pl.BlockSpec(shape, lambda *_: (0,) * len(shape), pipeline_mode=pl.Buffered(1))


def turned_of(a):
    return a.astype(F32).T.astype(BF16)


def norm_kernel(x, a, a_t):
    out = normed(x[...])
    a[...] = out
    a_t[...] = turned_of(out)


def turn_kernel(x, x_t):
    x_t[...] = turned_of(x[...])


def back_norm_kernel(by_a, h, by_h, out, out_t):
    new = by_h[...] + jax.vjp(normed, h[...])[1](by_a[...])[0]
    out[...] = new
    out_t[...] = turned_of(new)


def by_rows(kernel, kinds, *arrays, bm=512):
    m, n = arrays[0].shape
    straight, across = pl.BlockSpec((bm, n), lambda i: (i, 0)), pl.BlockSpec((n, bm), lambda i: (0, i))
    return call(
        kernel, [shaped((n, m) if kind == "t" else (m, n)) for kind in kinds], (m // bm,), [straight] * len(arrays),
        [across if kind == "t" else straight for kind in kinds], 10**9, 2 * m * n * (len(arrays) + len(kinds)),
    )(*arrays)


def gate_up_kernel(number, width, outputs, at, a_far, *refs):
    sources, outs, (buf, sem) = (refs[:4], refs[4:8]), refs[-4 - outputs : -4], refs[-4:-2]
    a, a_sem = refs[-2:]
    a_copy = pltpu.make_async_copy(a_far, a, a_sem)
    by_gate, by_up, hidden = outs[:3]
    t = pl.program_id(0)
    tile = hidden.shape[1]
    rows = buf.shape[2] // 4
    here = lambda first: pl.ds(pl.multiple_of(first, 128), tile)

    def copies(t):
        slot = lax.rem(t, 2)
        out = []
        for p in range(2):
            own, own_c, rx, rx_c = sources[p]
            cut = [own.at[number, :, here(at[4] * width + t * tile)], own_c.at[number, :, here(at[4] * width + t * tile)]]
            cut += [rx.at[:, here(t * tile)], rx_c.at[:, here(t * tile)]]
            for k, src in enumerate(cut):
                dst = buf.at[slot, p, pl.ds(pl.multiple_of(at[k] * rows, rows), rows)]
                out.append(pltpu.make_async_copy(src, dst, sem.at[slot, p, k]))
        return out

    @pl.when(t == 0)
    def _():
        a_copy.start()
        for one in copies(t):
            one.start()

    @pl.when(t + 1 < pl.num_programs(0))
    def _():
        for one in copies(t + 1):
            one.start()

    @pl.when(t == 0)
    def _():
        a_copy.wait()

    for one in copies(t):
        one.wait()
    slot = lax.rem(t, 2)
    for p, whole in enumerate(outs[3:]):
        whole[...] = buf[slot, p]
    g = jnp.dot(a[...], buf[slot, 0], preferred_element_type=F32)
    u = jnp.dot(a[...], buf[slot, 1], preferred_element_type=F32)
    s = jax.nn.sigmoid(g)
    silu = g * s
    by_gate[...] = u * (s + silu * (1 - s))
    by_up[...] = silu
    hidden[...] = (silu * u).astype(BF16)


def gate_up(number, at, a, gates, ups, before=()):
    m, k = a.shape
    n, width = gates[0].shape[2], gates[2].shape[1]
    bn = 256
    tiles = width // bn
    any_space = pl.BlockSpec(memory_space=pl.ANY)
    place = lambda t, at: (0, at[4] * tiles + t)
    out, w = pl.BlockSpec((m, bn), place), pl.BlockSpec((k, bn), place)
    return pl.pallas_call(
        functools.partial(gate_up_kernel, number, width, 5 if number else 3),
        out_shape=[shaped((m, n), F32), shaped((m, n), F32), shaped((m, n))] + [shaped((k, n))] * (2 if number else 0),
        grid_spec=pltpu.PrefetchScalarGridSpec(
            num_scalar_prefetch=1,
            grid=(tiles,),
            in_specs=[any_space] * (9 + len(before)),
            out_specs=[out] * 3 + [w] * (2 if number else 0),
            scratch_shapes=[
                pltpu.VMEM((2, 2, k, bn), BF16),
                pltpu.SemaphoreType.DMA((2, 2, 4)),
                pltpu.VMEM((m, k), BF16),
                pltpu.SemaphoreType.DMA,
            ],
        ),
        input_output_aliases={10 + i: i for i in range(len(before))},
        compiler_params=pltpu.CompilerParams(vmem_limit_bytes=VMEM),
        cost_estimate=pl.CostEstimate(flops=4 * m * width * k, bytes_accessed=10 * m * width + 4 * k * width, transcendentals=FREE),
        name="gate_up",
    )(at, a, *gates, *ups, *before)


def arriving(number, rows, pieces, buf, sem):
    own, own_c, rx, ry, rx_c, ry_c = pieces
    d, r = lax.axis_index("dp"), lax.axis_index("rep")
    half = rows // 2
    own_i, core_i, x_i, xc_i = others(d)
    at = lambda i, n: buf.at[pl.ds(pl.multiple_of(i, 16), n)]
    moves = [
        (own.at[number], at(own_i * rows, rows)),
        (own_c.at[number], at(core_i * rows, rows)),
        (rx, at(x_i * rows + r * half, half)),
        (ry, at(x_i * rows + (1 - r) * half, half)),
        (rx_c, at(xc_i * rows + r * half, half)),
        (ry_c, at(xc_i * rows + (1 - r) * half, half)),
    ]
    return [pltpu.make_async_copy(src, dst, sem.at[k]) for k, (src, dst) in enumerate(moves)]


def down_kernel(number, rows, hidden, x, *refs):
    pieces, (h, a, a_t, whole, buf, sem, out_sem) = refs[:6], refs[6:]
    i = pl.program_id(0)
    put = pltpu.make_async_copy(buf, whole, out_sem)

    @pl.when(i == 0)
    def _():
        ins = arriving(number, rows, pieces, buf, sem)
        for one in ins:
            one.start()
        for one in ins:
            one.wait()
        put.start()

    out = x[...] + jnp.dot(hidden[...], buf[...], preferred_element_type=F32).astype(BF16)
    h[...] = out
    out = normed(out)
    a[...] = out
    a_t[...] = turned_of(out)

    @pl.when(i == pl.num_programs(0) - 1)
    def _():
        put.wait()


def down(number, hidden, x, pieces, bm=512):
    m, k = hidden.shape
    n, rows = pieces[0].shape[2], pieces[0].shape[1]
    out = pl.BlockSpec((bm, n), lambda i: (i, 0))
    any_space = pl.BlockSpec(memory_space=pl.ANY)
    return call(
        functools.partial(down_kernel, number, rows), [shaped((m, n))] * 2 + [shaped((n, m)), shaped((k, n))], (m // bm,),
        [pl.BlockSpec((bm, k), lambda i: (i, 0)), out] + [any_space] * 6,
        [out] * 2 + [pl.BlockSpec((n, bm), lambda i: (0, i)), any_space], 2 * m * n * k, 4 * k * n + 2 * m * k,
        scratch=[pltpu.VMEM((k, n), BF16), pltpu.SemaphoreType.DMA((6,)), pltpu.SemaphoreType.DMA],
    )(hidden, x, *pieces)


NT = (((1,), (1,)), ((), ()))


def by_hidden_kernel(dy, w, gate, up, dg, du):
    by = lax.dot_general(dy[...], w[...], NT, preferred_element_type=F32).astype(BF16).astype(F32)
    dg[...] = (by * gate[...]).astype(BF16)
    du[...] = (by * up[...]).astype(BF16)


def by_hidden(dy, w, gate, up, bn=512):
    m, k = dy.shape
    n = w.shape[0]
    out = pl.BlockSpec((m, bn), lambda j: (0, j))
    return call(
        by_hidden_kernel, [shaped((m, n))] * 2, (n // bn,),
        [resident((m, k)), pl.BlockSpec((bn, k), lambda j: (j, 0)), out, out], [out] * 2, 2 * m * n * k, 12 * m * n,
    )(dy, w, gate, up)


def by_hidden_pieces_kernel(number, rows, dy, gate, up, *refs):
    pieces, (dg, du, buf, sem) = refs[:6], refs[6:]
    j, bn = pl.program_id(0), dg.shape[1]

    @pl.when(j == 0)
    def _():
        ins = arriving(number, rows, pieces, buf, sem)
        for one in ins:
            one.start()
        for one in ins:
            one.wait()

    w = buf[pl.ds(pl.multiple_of(j * bn, bn), bn), :]
    by = lax.dot_general(dy[...], w, NT, preferred_element_type=F32).astype(BF16).astype(F32)
    dg[...] = (by * gate[...]).astype(BF16)
    du[...] = (by * up[...]).astype(BF16)


def by_hidden_pieces(number, dy, pieces, gate, up, bn=512):
    m, k = dy.shape
    n, rows = gate.shape[1], pieces[0].shape[1]
    out = pl.BlockSpec((m, bn), lambda j: (0, j))
    return call(
        functools.partial(by_hidden_pieces_kernel, number, rows), [shaped((m, n))] * 2, (n // bn,),
        [resident((m, k)), out, out] + [pl.BlockSpec(memory_space=pl.ANY)] * 6, [out] * 2, 2 * m * n * k, 12 * m * n,
        scratch=[pltpu.VMEM((n, k), BF16), pltpu.SemaphoreType.DMA((6,))],
    )(dy, gate, up, *pieces)


def by_a_kernel(dg, du, wg, wu, out):
    one = lax.dot_general(dg[...], wg[...], NT, preferred_element_type=F32).astype(BF16)
    two = lax.dot_general(du[...], wu[...], NT, preferred_element_type=F32).astype(BF16)
    out[...] = one + two


def by_a(dg, du, wg, wu, bm=1024, bn=512):
    m, k = dg.shape
    n = wg.shape[0]
    lhs = pl.BlockSpec((bm, k), lambda i, j: (i, 0))
    w = pl.BlockSpec((bn, k), lambda i, j: (j, 0))
    return call(
        by_a_kernel, shaped((m, n)), (m // bm, n // bn), [lhs, lhs, w, w], pl.BlockSpec((bm, bn), lambda i, j: (i, j)),
        4 * m * n * k, 4 * m * k + 4 * n * k * (m // bm),
    )(dg, du, wg, wu)


TILE = 512


def exchange(d, src, dst, send_sem, recv_sem):
    return pltpu.make_async_remote_copy(
        src_ref=src, dst_ref=dst, send_sem=send_sem, recv_sem=recv_sem, device_id={"dp": others(d)[1]}, device_id_type=pl.DeviceIdType.MESH
    )


def greet(d):
    barrier = pltpu.get_barrier_semaphore()
    pl.semaphore_signal(barrier, inc=1, device_id={"dp": others(d)[1]}, device_id_type=pl.DeviceIdType.MESH)
    pl.semaphore_wait(barrier, 1)


def term_rows_kernel(left, right, send, kept, three, full, there, send_sem, recv_sem):
    d = lax.axis_index("dp")
    _, core_i, x_i, xc_i = others(d)
    rows, tile = send.shape
    tiles = full.shape[1] // tile
    j = pl.program_id(0)
    cols = lambda k: pl.ds(pl.multiple_of(k * tile, tile), tile)

    def copies(k):
        return [
            exchange(d, full.at[pl.ds(n * rows, rows), cols(k)], there.at[n, :, cols(k)], send_sem.at[n, k], recv_sem.at[n, k])
            for n in range(2)
        ]

    @pl.when(j == 0)
    def _():
        greet(d)
        for n, i in enumerate((core_i, xc_i, x_i)):
            three[pl.ds(n * rows, rows), :] = left[pl.ds(pl.multiple_of(i * rows, rows), rows), :]

    @pl.when((j >= 1) & (j <= tiles))
    def _():
        for one in copies(j - 1):
            one.start()

    @pl.when(j < tiles)
    def _():
        full[:, cols(j)] = jnp.dot(three[...], right[...], preferred_element_type=F32).astype(BF16)

    @pl.when(j >= 2)
    def _():
        k = j - 2
        for one in copies(k):
            one.wait()
        kept[...] = there[0, :, cols(k)]
        send[...] = (full[pl.ds(2 * rows, rows), cols(k)].astype(F32) + there[1, :, cols(k)].astype(F32)).astype(BF16)


def term_rows(left, right):
    m, k = left.shape
    n, rows, tiles = right.shape[1], m // 4, right.shape[1] // TILE
    out = pl.BlockSpec((rows, TILE), lambda j: (0, jnp.maximum(j - 2, 0)))
    return pl.pallas_call(
        term_rows_kernel,
        out_shape=[shaped((rows, n)), shaped((rows, n))],
        grid=(tiles + 2,),
        in_specs=[resident((m, k)), pl.BlockSpec((k, TILE), lambda j: (0, jnp.minimum(j, tiles - 1)))],
        out_specs=[out, out],
        scratch_shapes=[
            pltpu.VMEM((3 * rows, k), BF16),
            pltpu.VMEM((3 * rows, n), BF16),
            pltpu.VMEM((2, rows, n), BF16),
            pltpu.SemaphoreType.DMA((2, tiles)),
            pltpu.SemaphoreType.DMA((2, tiles)),
        ],
        compiler_params=pltpu.CompilerParams(vmem_limit_bytes=VMEM, collective_id=FREE, has_side_effects=True),
        cost_estimate=pl.CostEstimate(flops=3 * m * n * k // 2, bytes_accessed=2 * (m * k + k * n + m * n), transcendentals=FREE),
        name="term_rows",
    )(left, right)


def count(squares, g):
    @pl.when(pl.program_id(0) == 0)
    def _():
        squares[0, 0] = 0.0

    squares[0, 0] += jnp.sum(g * g)


def own_rows_kernel(at, left, right, kept, out):
    out[...] = jnp.dot(left[...], right[...], preferred_element_type=F32) + kept[...].astype(F32)


def own_rows_end_kernel(at, left, right, kept, arrived, out, squares):
    total = jnp.dot(left[...], right[...], preferred_element_type=F32) + kept[...].astype(F32)
    g = (total + arrived[...].astype(F32)).astype(BF16)
    out[...] = g
    count(squares, g.astype(F32))


def own_rows(at, left, right, kept, arrived=None):
    m, k = left.shape
    n, rows = right.shape[1], m // 4
    out = pl.BlockSpec((rows, TILE), lambda j, at: (0, j))
    ins = [pl.BlockSpec((rows, k), lambda j, at: (at[0], 0)), pl.BlockSpec((k, TILE), lambda j, at: (0, j)), out]
    if arrived is None:
        return call(own_rows_kernel, shaped((rows, n), F32), (n // TILE,), ins, out, 2 * rows * n * k, 2 * k * n, at)(at, left, right, kept)
    return call(
        own_rows_end_kernel, [shaped((rows, n)), shaped((1, 1), F32)], (n // TILE,), ins + [out],
        [out, pl.BlockSpec(memory_space=pltpu.SMEM)], 2 * rows * n * k, 2 * k * n, at,
    )(at, left, right, kept, arrived)


def ended_kernel(elements, own, arrived, before, out, factor, acc, mine, got, send_sem, recv_sem):
    d = lax.axis_index("dp")
    j, last = pl.program_id(0), pl.num_programs(0) - 1
    peers = [lax.rem(d + k, 4) for k in (1, 2, 3)]
    barrier = pltpu.get_barrier_semaphore()

    @pl.when(j == 0)
    def _():
        for peer in peers:
            pl.semaphore_signal(barrier, inc=1, device_id={"dp": peer}, device_id_type=pl.DeviceIdType.MESH)
        acc[...] = jnp.zeros_like(acc)

    g = (own[...] + arrived[...].astype(F32)).astype(BF16)
    out[...] = g
    g = g.astype(F32)
    acc[...] += jnp.sum((g * g).reshape(g.shape[0] // 8, 8, g.shape[1]), axis=0)

    @pl.when(j == last)
    def _():
        mine[...] = jnp.full(mine.shape, jnp.sum(acc[...]) + before[0, 0], F32)
        pl.semaphore_wait(barrier, 3)
        copies = [
            pltpu.make_async_remote_copy(
                src_ref=mine, dst_ref=got.at[k], send_sem=send_sem.at[k], recv_sem=recv_sem.at[k],
                device_id={"dp": peer}, device_id_type=pl.DeviceIdType.MESH,
            )
            for k, peer in enumerate(peers)
        ]
        for one in copies:
            one.start()
        for one in copies:
            one.wait()
        squares = mine[...] + got[0] + got[1] + got[2]
        factor[...] = jnp.minimum(1.0, 0.5 * lax.rsqrt(squares / elements + 1e-30))


ENDED = 896


def ended(own, arrived, before, elements):
    m, n = own.shape
    spec = pl.BlockSpec((m, ENDED), lambda j: (0, j))
    return pl.pallas_call(
        functools.partial(ended_kernel, elements),
        out_shape=[shaped((m, n)), shaped((8, 128), F32)],
        grid=(n // ENDED,),
        in_specs=[spec, spec, pl.BlockSpec(memory_space=pltpu.SMEM)],
        out_specs=[spec, pl.BlockSpec((8, 128), lambda j: (0, 0))],
        scratch_shapes=[
            pltpu.VMEM((8, ENDED), F32),
            pltpu.VMEM((8, 128), F32),
            pltpu.VMEM((3, 8, 128), F32),
            pltpu.SemaphoreType.DMA((3,)),
            pltpu.SemaphoreType.DMA((3,)),
        ],
        compiler_params=pltpu.CompilerParams(vmem_limit_bytes=VMEM, collective_id=2, has_side_effects=True),
        cost_estimate=pl.CostEstimate(flops=4 * m * n, bytes_accessed=8 * m * n, transcendentals=FREE),
        name="ended",
    )(own, arrived, before)


def term_columns_kernel(left, right, send, own, full, there, send_sem, recv_sem):
    d = lax.axis_index("dp")
    x, c = d // 2, d % 2
    wide = send.shape[1]
    tile = right.shape[1]
    tiles = full.shape[1] // tile
    j = pl.program_id(0)

    def pieces(s):
        first, end = s * wide, (s + 1) * wide
        if s < 3:
            return [(first, wide, (end - 1) // tile)]
        cut = (tiles - 1) * tile
        return [(first, cut - first, (cut - 1) // tile), (cut, end - cut, tiles - 1)]

    def copies(s):
        out = []
        for p, (first, width, last) in enumerate(pieces(s)):
            n = jnp.where(x == s // 2, 0, 1)
            dst = there.at[n, :, pl.ds(first - s * wide, width)]
            out.append((last, exchange(d, full.at[:, pl.ds(first, width)], dst, send_sem.at[s, p], recv_sem.at[s, p])))
        return out

    @pl.when(j == 0)
    def _():
        greet(d)

    for s in range(4):
        for last, one in copies(s):

            @pl.when((j == last + 1) & (c != s % 2))
            def _(one=one):
                one.start()

    @pl.when(j < tiles)
    def _():
        here = pl.ds(pl.multiple_of(j * tile, tile), tile)
        full[:, here] = jnp.dot(left[...], right[...], preferred_element_type=F32).astype(BF16)

    @pl.when(j == tiles + 1)
    def _():
        for s in range(4):
            for last, one in copies(s):

                @pl.when(c != s % 2)
                def _(one=one):
                    one.wait_send()

                @pl.when(c == s % 2)
                def _(one=one):
                    one.wait_recv()

            @pl.when((c == s % 2) & (x == s // 2))
            def _(s=s):
                own[...] = full[:, pl.ds(s * wide, wide)].astype(F32) + there[0].astype(F32)

            @pl.when((c == s % 2) & (x != s // 2))
            def _(s=s):
                send[...] = (full[:, pl.ds(s * wide, wide)].astype(F32) + there[1].astype(F32)).astype(BF16)


def term_columns(left, right):
    m, k = left.shape
    n, wide, tiles = right.shape[1], right.shape[1] // 4, right.shape[1] // TILE
    return pl.pallas_call(
        term_columns_kernel,
        out_shape=[shaped((m, wide)), shaped((m, wide), F32)],
        grid=(tiles + 2,),
        in_specs=[resident((m, k)), pl.BlockSpec((k, TILE), lambda j: (0, jnp.minimum(j, tiles - 1)))],
        out_specs=[pl.BlockSpec((m, wide), lambda j: (0, 0))] * 2,
        scratch_shapes=[pltpu.VMEM((m, n), BF16), pltpu.VMEM((2, m, wide), BF16), pltpu.SemaphoreType.DMA((4, 2)), pltpu.SemaphoreType.DMA((4, 2))],
        compiler_params=pltpu.CompilerParams(vmem_limit_bytes=VMEM, collective_id=1, has_side_effects=True),
        cost_estimate=pl.CostEstimate(flops=2 * m * n * k, bytes_accessed=2 * (m * k + k * n + m * n), transcendentals=FREE),
        name="term_columns",
    )(left, right)


def turned_kernel(own, arrived, out, squares):
    g = (own[...] + arrived[...].astype(F32)).astype(BF16).astype(F32)
    count(squares, g)
    out[...] = g.T.astype(BF16)


def turned(own, arrived):
    m, n = own.shape
    bn = 128
    spec = pl.BlockSpec((m, bn), lambda j: (0, j))
    g, squares = pl.pallas_call(
        turned_kernel,
        out_shape=[shaped((n, m)), shaped((1, 1), F32)],
        grid=(n // bn,),
        in_specs=[spec, spec],
        out_specs=[pl.BlockSpec((bn, m), lambda j: (j, 0)), pl.BlockSpec(memory_space=pltpu.SMEM)],
        compiler_params=pltpu.CompilerParams(vmem_limit_bytes=VMEM),
        cost_estimate=pl.CostEstimate(flops=4 * m * n, bytes_accessed=8 * m * n, transcendentals=FREE),
        name="turned",
    )(own, arrived)
    return g, squares


def solution(mesh):
    def step(x, dy, *arrays):
        weights, m, v = (arrays[i : i + 3] for i in (0, 3, 6))
        d, r = lax.axis_index("dp"), lax.axis_index("rep")
        own_i, core_i, x_i, xc_i = others(d)
        layers = weights[0].shape[0]

        from_core = [lax.ppermute(w, "dp", OVER_CORE) for w in weights]

        def across(i, number):
            rows, cols = weights[i].shape[1:]
            if i == 2:
                mine = lax.dynamic_slice(weights[i], (number, r * (rows // 2), 0), (1, rows // 2, cols))[0]
            else:
                mine = lax.dynamic_slice(weights[i], (number, 0, r * (cols // 2)), (1, rows, cols // 2))[0]
            return lax.ppermute(mine, "dp", OVER_X)

        halves = {(i, number): across(i, number) for number in range(layers) for i in range(3)}

        def first(i, number, *behind):
            rx = halves[i, number]
            if behind:
                rx = lax.optimization_barrier((rx, *behind))[0]
            return lax.ppermute(rx, "dp", OVER_CORE)

        def second(i, number, *behind):
            rx = halves[i, number]
            if behind:
                rx = lax.optimization_barrier((rx, *behind))[0]
            ry = lax.ppermute(rx, "rep", OVER_Y)
            return ry, lax.ppermute(ry, "dp", OVER_CORE)

        def down_pieces(number, behind):
            ry, ry_c = second(2, number, behind)
            return weights[2], from_core[2], halves[2, number], ry, first(2, number), ry_c

        last = []

        def ordered(*some):
            out = lax.optimization_barrier((*some, *last))[: len(some)] if last else some
            return out[0] if len(some) == 1 else out

        def noted(one):
            last[:] = [one]
            return one

        at = jnp.stack([own_i, core_i, x_i, xc_i, r]).astype(jnp.int32)
        at_b = jnp.stack([own_i, core_i, x_i, xc_i, 1 - r]).astype(jnp.int32)

        def ab(number, a, behind):
            arrived = [(weights[i], from_core[i], halves[i, number], first(i, number, *behind[i])) for i in (0, 1)]
            outs = gate_up(number, at, a, *arrived)
            return outs, [(weights[i], from_core[i], *second(i, number, *behind[i])) for i in (0, 1)]

        a0, a0_t = by_rows(norm_kernel, " t", x[0])
        (dy_t,) = by_rows(turn_kernel, "t", lax.optimization_barrier((dy[0], a0, halves[0, 0]))[0])
        a0, a0_t, dy_t = lax.optimization_barrier((a0, a0_t, dy_t))
        outs, arrived = ab(0, a0, ((), ()))
        pieces0 = down_pieces(0, outs[2])
        gate0, up0, hidden0 = gate_up(0, at_b, a0, *arrived, outs)
        h1, a1, a1_t, w_down0 = down(0, hidden0, x[0], pieces0)
        outs, arrived = ab(1, a1, ((hidden0,), (h1,)))
        pieces1 = down_pieces(1, outs[2])
        gate1, up1, hidden1, w_gate1, w_up1 = gate_up(1, at_b, a1, *arrived, outs)
        noted(hidden1)

        mine, late = [[None] * 3 for _ in range(layers)], {}

        def term(i, number, kernel, left, right):
            send, kept = kernel(left, ordered(right))
            noted(send)
            late[i, number] = lax.ppermute(send, "dp", OVER_X), kept, left, right

        term(2, 1, term_columns, dy_t, hidden1)
        by_gate, by_up = by_hidden_pieces(1, ordered(dy[0]), pieces1, gate1, up1)
        noted(by_gate)
        term(0, 1, term_rows, a1_t, by_gate)
        term(1, 1, term_rows, a1_t, by_up)
        by_in = by_a(ordered(by_gate), by_up, w_gate1, w_up1)
        by_h, by_h_t = by_rows(back_norm_kernel, " t", by_in, h1, dy[0])
        noted(by_h)
        term(2, 0, term_columns, by_h_t, hidden0)
        by_gate, by_up = by_hidden(ordered(by_h), w_down0, gate0, up0)
        noted(by_gate)
        term(0, 0, term_rows, a0_t, by_gate)
        term(1, 0, term_rows, a0_t, by_up)
        _, kept, left, right = late[1, 0]
        last_own = noted(own_rows(at, left, ordered(right), kept))
        squares = 0.0
        for i, number in ((0, 1), (1, 1), (2, 1), (2, 0), (0, 0)):
            from_x, kept, left, right = late[i, number]
            if i == 2:
                g, more = turned(ordered(kept), from_x)
            else:
                g, more = own_rows(at, left, ordered(right), kept, from_x)
            mine[number][i] = noted(g)
            squares += more
        count = 4 * sum(w.size for w in weights)
        mine[0][1], factor = ended(ordered(last_own), late[1, 0][0], squares, count)
        factor = factor[0, 0]
        new = []
        for i in range(3):
            g = jnp.stack([mine[number][i] for number in range(layers)]).astype(F32) * factor
            new.append(adamw(weights[i].astype(F32), m[i], v[i], g))
        return tuple(one[which] for which in range(3) for one in new)

    states, cut = P(("rep", "dp"), None, None), P(None, "dp", None)
    return jax.shard_map(
        step,
        mesh=mesh,
        in_specs=(states, states) + (cut,) * 9,
        out_specs=(P("rep", "dp", None),) * 9,
        check_vma=False,
    )
```
